32 devices in a mesh: dp: 16 (over z, y, x), tp: 2 (over core).
Axes of the slice: x: 2, y: 2, z: 4, core: 2. Of those that a mesh axis runs over, the one named last changes fastest.
Arguments:
- tokens: bfloat16 [2048, 4096], P('dp', 'tp'), may hold values from -6 to 6
- norm_gain: float32 [4096], replicated, may hold values from 0.1 to 1.9
- w_query: bfloat16 [4096, 2048], P(None, 'tp'), may hold values from -0.09375 to 0.09375
- w_key: bfloat16 [4096, 512], P(None, 'tp'), may hold values from -0.09375 to 0.09375
- w_value: bfloat16 [4096, 512], P(None, 'tp'), may hold values from -0.09375 to 0.09375
- w_out: bfloat16 [2048, 4096], P('tp'), may hold values from -0.125 to 0.125
- mlp_gain: float32 [4096], replicated, may hold values from 0.1 to 1.9
- w_gate: bfloat16 [4096, 7168], P(None, 'tp'), may hold values from -0.09375 to 0.09375
- w_up: bfloat16 [4096, 7168], P(None, 'tp'), may hold values from -0.09375 to 0.09375
- w_down: bfloat16 [7168, 4096], P('tp'), may hold values from -0.0625 to 0.0625
- kv_pool: bfloat16 [1024, 2, 4, 128, 128], P('dp', None, 'tp'), may hold values from -160 to 160, as said below
- prefix_len: int32 [16], replicated, may hold values from 1024 to 8192, as said below
- page_owner: int32 [16, 64], replicated, may hold values from -1 to 15, as said below
- page_slot: int32 [16, 64], replicated, may hold values from -1 to 63, as said below
- serving: int32 [16], replicated, may hold values from 0 to 15, each once
Outputs:
- context: bfloat16 [2048, 2048], P('dp', 'tp')
- layer_out: bfloat16 [2048, 4096], P('dp', 'tp')
The draws below stay inside these ranges and needn't reach their ends.
Inputs may be any that keep to these rules, and one draw needn't show every extreme that they name: `prefix_len`: prefix lengths lie between 1024 and 8192; some request has exactly 8192 cached tokens and some exactly 1024. page_owner[r, p] names an index along dp for p < ceil(prefix_len[r] / 128) and is -1 after; no index holds more than 4 pages of one request, and for every request some index holds exactly 4 of its pages. page_slot[r, p] lies in 0 to 63 where page_owner[r, p] is not -1 and is -1 where it is; no two pages share the same holder and slot. serving is a permutation of the requests. `kv_pool`: cached keys and values, each page with an offset of its own.
All inputs are finite; a program needn't handle non-finite values.
Results may differ from the reference program's by a relative error of at most 0.014.
The reference program's roundings to bfloat16 on the way count: a program that leaves them out, or rounds other values in their place, can miss the bound.
Values may be sent and summed in bfloat16 or wider, within the bound.
A program may use at most 256 MiB of HBM per device.

```python
import math
import jax
import jax.numpy as jnp
from jax import lax

D = 4096
HD = 128
QH = 16
KVH = 4
FF_WIN = 7168
PAGE = 128
MAXP = 64
NEW = 128
REQUESTS = 16
TOKENS = 2048
SLOTS = 1024
PER_OWNER = 4
N_DP = 16
N_TP = 2


def permute_one(sub_key):
    return jax.random.permutation(sub_key, MAXP)


def layout(key):
    shortest = PAGE * MAXP // 8
    longest = PAGE * MAXP
    lengths = jax.random.randint(jax.random.fold_in(key, 101), (REQUESTS,), shortest, longest + 1)
    top_pick = jax.random.randint(jax.random.fold_in(key, 102), (), 0, REQUESTS)
    low_pick = (top_pick + jax.random.randint(jax.random.fold_in(key, 103), (), 1, REQUESTS)) % REQUESTS
    request_ids = jnp.arange(REQUESTS)
    lengths = jnp.where(request_ids == top_pick, longest, jnp.where(request_ids == low_pick, shortest, lengths))
    page_count = (lengths + PAGE - 1) // PAGE
    shifts = jax.random.permutation(jax.random.fold_in(key, 104), REQUESTS)
    relabel = jax.random.permutation(jax.random.fold_in(key, 105), REQUESTS)
    slot_orders = jax.vmap(permute_one)(jax.random.split(jax.random.fold_in(key, 106), REQUESTS))
    page_ids = jnp.arange(MAXP)
    block_ids = page_ids // PER_OWNER
    owner_spot = (block_ids[None, :] + shifts[:, None]) % REQUESTS
    owners = jnp.take(relabel, owner_spot)
    slot_ids = slot_orders[owners, page_ids[None, :]]
    in_prefix = page_ids[None, :] < page_count[:, None]
    return (lengths.astype(jnp.int32), jnp.where(in_prefix, owners, -1).astype(jnp.int32), jnp.where(in_prefix, slot_ids, -1).astype(jnp.int32))


def draw_prefix_len(key, part):
    return layout(key)[0]


def draw_page_owner(key, part):
    return layout(key)[1]


def draw_page_slot(key, part):
    return layout(key)[2]


def draw_kv_pool(key, part):
    base_key = jax.random.fold_in(key, 7)
    page_key = jax.random.fold_in(key, 8)
    full_shape = (SLOTS, 2, KVH, PAGE, HD)
    page_shape = (SLOTS, 2, KVH, 1, HD)
    base = jax.random.normal(base_key, full_shape, jnp.float32)
    offset = jax.random.normal(page_key, page_shape, jnp.float32)
    return (base + offset).astype(jnp.bfloat16)


def steps_of(key, dims, shards, smallest, largest):
    factor_of, own = 1.0, jax.random.fold_in(key, 6)
    for dim, blocks in shards:
        heights = jnp.exp(jax.random.uniform(jax.random.fold_in(own, dim), (blocks,), jnp.float32, smallest / len(shards), largest / len(shards)))
        factor_of = factor_of * jnp.repeat(heights, dims[dim] // blocks).reshape([-1 if axis == dim else 1 for axis in range(len(dims))])
    return factor_of


def normal_values(stream_key, extent, scale, limit, shards=(), held_as=jnp.bfloat16):
    level = steps_of(stream_key, extent, shards, -0.22, 0.18) if shards else 1.0
    entries = jax.random.normal(stream_key, extent, jnp.float32) * scale * level
    return jnp.minimum(jnp.maximum(entries, -limit), limit).astype(held_as)


def setup_inputs(seed: int = 0) -> dict:
    arg_keys = jax.random.split(jax.random.key(seed), 16)
    tokens = normal_values(arg_keys[0], (TOKENS, D), 1.0, 6.0, ((0, 16), (1, 2)))
    norm_gain = jnp.clip(1.0 + 0.18 * jax.random.normal(arg_keys[1], (D,), jnp.float32), 0.1, 1.9)
    w_query = normal_values(arg_keys[2], (D, QH * HD), D ** -0.5, 0.09375, ((1, 2),))
    w_key = normal_values(arg_keys[3], (D, KVH * HD), D ** -0.5, 0.09375, ((1, 2),))
    w_value = normal_values(arg_keys[4], (D, KVH * HD), D ** -0.5, 0.09375, ((1, 2),))
    w_out = normal_values(arg_keys[5], (QH * HD, D), (QH * HD) ** -0.5, 0.125, ((0, 2),))
    mlp_gain = jnp.clip(1.0 + 0.18 * jax.random.normal(arg_keys[6], (D,), jnp.float32), 0.1, 1.9)
    w_gate = normal_values(arg_keys[7], (D, FF_WIN), D ** -0.5, 0.09375, ((1, 2),))
    w_up = normal_values(arg_keys[8], (D, FF_WIN), D ** -0.5, 0.09375, ((1, 2),))
    w_down = normal_values(arg_keys[9], (FF_WIN, D), FF_WIN ** -0.5, 0.0625, ((0, 2),))
    kv_pool = draw_kv_pool(jax.random.fold_in(arg_keys[15], 71), 0)
    prefix_len = draw_prefix_len(jax.random.fold_in(arg_keys[15], 71), 0)
    page_owner = draw_page_owner(jax.random.fold_in(arg_keys[15], 71), 0)
    page_slot = draw_page_slot(jax.random.fold_in(arg_keys[15], 71), 0)
    serving = jax.random.permutation(arg_keys[14], REQUESTS).astype(jnp.int32)
    return {"tokens": tokens, "norm_gain": norm_gain, "w_query": w_query, "w_key": w_key, "w_value": w_value, "w_out": w_out, "mlp_gain": mlp_gain, "w_gate": w_gate, "w_up": w_up, "w_down": w_down, "kv_pool": kv_pool, "prefix_len": prefix_len, "page_owner": page_owner, "page_slot": page_slot, "serving": serving}


EPS = 1e-05
THETA = 500000.0
NEG = -1e+30

def rms_normalize(values, gain):
    as_f32 = values.astype(jnp.float32)
    factor = lax.rsqrt(lax.optimization_barrier(jnp.mean(as_f32 * as_f32, axis=-1, keepdims=True)) + EPS)
    return (as_f32 * factor * gain).astype(jnp.bfloat16)

def rotate(vectors, positions):
    half_dim = vectors.shape[-1] // 2
    freq_index = jnp.arange(half_dim, dtype=jnp.float32)
    inverse = jnp.power(jnp.float32(THETA), -2.0 * freq_index / vectors.shape[-1])
    angles = positions.astype(jnp.float32)[:, None] * inverse[None, :]
    cosine = jnp.cos(angles)[:, None, :]
    sine = jnp.sin(angles)[:, None, :]
    first = vectors[..., :half_dim]
    second = vectors[..., half_dim:]
    return jnp.concatenate([first * cosine - second * sine, second * cosine + first * sine], axis=-1)

def attend(queries, keys_all, values_all, length, new_tokens):
    row_count = queries.shape[1]
    prefix_slots = keys_all.shape[1] - new_tokens
    scores = jnp.einsum('hqd,hkd->hqk', queries.astype(jnp.float32), keys_all.astype(jnp.float32))
    scores = scores / math.sqrt(queries.shape[2])
    row_token = jnp.arange(row_count, dtype=jnp.int32) % new_tokens
    prefix_ok = jnp.arange(prefix_slots, dtype=jnp.int32) < length
    causal = jnp.arange(new_tokens, dtype=jnp.int32)[None, :] <= row_token[:, None]
    allowed = jnp.concatenate([jnp.broadcast_to(prefix_ok[None, :], (row_count, prefix_slots)), causal], axis=1)
    scores = jnp.where(allowed[None], scores, NEG)
    highest = lax.optimization_barrier(jnp.max(scores, axis=-1, keepdims=True))
    expo = jnp.exp(scores - highest)
    weights = (expo / lax.optimization_barrier(jnp.sum(expo, axis=-1, keepdims=True))).astype(jnp.bfloat16)
    result = jnp.einsum('hqk,hkd->hqd', weights.astype(jnp.float32), values_all.astype(jnp.float32))
    return result.astype(jnp.bfloat16)

def rounded_blocks(left, right, blocks):
    block_size = left.shape[1] // blocks
    running = jnp.zeros((left.shape[0], right.shape[1]), jnp.float32)
    for index in range(blocks):
        partial_sum = jnp.dot(left[:, index * block_size:(index + 1) * block_size], right[index * block_size:(index + 1) * block_size], preferred_element_type=jnp.float32)
        partial_sum = lax.optimization_barrier(partial_sum.astype(jnp.bfloat16))
        running = running + partial_sum.astype(jnp.float32)
    return running

def reference(tokens, norm_gain, w_query, w_key, w_value, w_out, mlp_gain, w_gate, w_up, w_down, kv_pool, prefix_len, page_owner, page_slot, serving):
    normed = rms_normalize(tokens, norm_gain)
    starts = jnp.take(prefix_len, serving.astype(jnp.int32))
    positions = (starts[:, None] + jnp.arange(NEW, dtype=jnp.int32)[None, :]).reshape(-1)
    queries = rotate(jnp.dot(normed, w_query, preferred_element_type=jnp.float32).reshape(TOKENS, QH, HD), positions).astype(jnp.bfloat16)
    new_keys = rotate(jnp.dot(normed, w_key, preferred_element_type=jnp.float32).reshape(TOKENS, KVH, HD), positions).astype(jnp.bfloat16)
    new_values = jnp.dot(normed, w_value, preferred_element_type=jnp.float32).astype(jnp.bfloat16).reshape(TOKENS, KVH, HD)
    shared = QH // KVH

    def one_group(items):
        group_q, group_k, group_v, request = items
        length = prefix_len[request]
        owner_row = page_owner[request]
        slot_row = page_slot[request]
        row_index = jnp.where(owner_row >= 0, owner_row * MAXP + slot_row, 0).astype(jnp.int32)
        pages = jnp.take(kv_pool, row_index, axis=0)
        keys_all = jnp.concatenate([pages[:, 0].transpose(1, 0, 2, 3).reshape(KVH, MAXP * PAGE, HD), group_k.transpose(1, 0, 2)], axis=1)
        values_all = jnp.concatenate([pages[:, 1].transpose(1, 0, 2, 3).reshape(KVH, MAXP * PAGE, HD), group_v.transpose(1, 0, 2)], axis=1)
        stacked = group_q.reshape(NEW, KVH, shared, HD).transpose(1, 2, 0, 3).reshape(KVH, shared * NEW, HD)
        result = attend(stacked, keys_all, values_all, length, NEW)
        return result.reshape(KVH, shared, NEW, HD).transpose(2, 0, 1, 3).reshape(NEW, QH * HD)
    context = lax.map(one_group, (queries.reshape(N_DP, NEW, QH, HD), new_keys.reshape(N_DP, NEW, KVH, HD), new_values.reshape(N_DP, NEW, KVH, HD), serving.astype(jnp.int32)))
    context = context.reshape(TOKENS, QH * HD)
    attn_sum = rounded_blocks(context, w_out, N_TP)
    stream = (tokens.astype(jnp.float32) + attn_sum).astype(jnp.bfloat16)
    mlp_in = rms_normalize(stream, mlp_gain)
    gate_act = jnp.dot(mlp_in, w_gate, preferred_element_type=jnp.float32)
    up_act = jnp.dot(mlp_in, w_up, preferred_element_type=jnp.float32)
    hidden = (jax.nn.silu(gate_act) * up_act).astype(jnp.bfloat16)
    mlp_sum = rounded_blocks(hidden, w_down, N_TP)
    layer_out = (stream.astype(jnp.float32) + mlp_sum).astype(jnp.bfloat16)
    return (context, layer_out)
```

```python
import functools
import math

import jax
import jax.numpy as jnp
from jax import lax
from jax.experimental import pallas as pl
from jax.experimental.pallas import tpu as pltpu
from jax.sharding import PartitionSpec as P

EPS = 1e-05
THETA = 500000.0
NEG = -1e30
LOG2E = 1.4426950408889634
MESH = pl.DeviceIdType.MESH
VMEM = pltpu.VMEM
VMEM_BUDGET = 66_800_000
TILE = 256


def xor(a, b, bits):
    out = 0
    for bit in range(bits):
        unit = 1 << bit
        out = out + lax.rem(lax.div(a, unit) + lax.div(b, unit), 2) * unit
    return out


def merge_stats(left, right):
    shared = left.shape[0] // 2
    top = jnp.maximum(left[:shared], right[:shared])
    factor_left = jnp.exp2(left[:shared] - top)
    factor_right = jnp.exp2(right[:shared] - top)
    count = left[shared:] * factor_left + right[shared:] * factor_right
    return jnp.concatenate([top, count], axis=0), factor_left, factor_right


def layer_kernel(
    plan,
    slot_ref,
    valid_ref,
    cos_ref,
    sin_ref,
    gain_ref,
    mlp_gain_ref,
    tokens_ref,
    wq_ref,
    wk_ref,
    wv_ref,
    wo_ref,
    wg_ref,
    wu_ref,
    wd_ref,
    kv_ref,
    context_ref,
    layer_ref,
    ring,
    kv_buf,
    tok_all,
    normed,
    q_all,
    new_k,
    new_v,
    part,
    stat,
    box,
    stat_box,
    attn_all,
    hidden,
    mlp_part,
    mlp_box,
    ring_sem,
    kv_sem,
    tok_sem,
    tok_send,
    tok_recv,
    q_send,
    q_recv,
    part_send,
    part_recv,
    stat_send,
    stat_recv,
    attn_send,
    attn_recv,
    mlp_send,
    mlp_recv,
):
    groups, ranks, kv_heads, per_owner = plan
    me = lax.axis_index("dp")
    rank = lax.axis_index("tp")
    bits = groups.bit_length() - 1
    planes = groups // 4
    rows, model = normed.shape
    share = tokens_ref.shape[1]
    width = q_all.shape[3]
    heads = q_all.shape[1]
    shared = heads // kv_heads
    page = kv_ref.shape[3]
    slots = ring.shape[0]
    units = wd_ref.shape[0]
    own_rows = wo_ref.shape[0]
    peers = [lax.rem(rank + 1 + t, ranks) for t in range(ranks - 1)]

    def slabs(total):
        step = math.gcd(total, TILE)
        return step, total // step

    q_width, q_tiles = slabs(wq_ref.shape[1])
    k_width, k_tiles = slabs(wk_ref.shape[1])
    g_width, g_tiles = slabs(units)
    d_width, d_tiles = slabs(share)
    d_tiles = d_tiles * ranks
    o_stack = model // own_rows
    o_cols = o_stack * TILE
    o_tiles = model // o_cols
    first_k = q_tiles
    first_v = first_k + k_tiles
    first_o = first_v + k_tiles
    first_g = first_o + o_tiles
    first_d = first_g + 2 * g_tiles
    last = first_d + d_tiles

    def slot_of(tile):
        return tile % slots if isinstance(tile, int) else lax.rem(tile, slots)

    def column_copy(source, start, step, tile):
        slot = slot_of(tile)
        count = source.shape[0]
        columns = pl.ds(pl.multiple_of(start, step), step)
        return pltpu.make_async_copy(
            source.at[:, columns],
            ring.at[slot, pl.ds(0, count), pl.ds(0, step)],
            ring_sem.at[slot],
        )

    def q_copy(i):
        return column_copy(wq_ref, i * q_width, q_width, i)

    def k_copy(i):
        return column_copy(wk_ref, i * k_width, k_width, first_k + i)

    def v_copy(i):
        return column_copy(wv_ref, i * k_width, k_width, first_v + i)

    def gate_copy(i, which):
        return column_copy((wg_ref, wu_ref)[which], i * g_width, g_width, first_g + 2 * i + which)

    def down_copy(i):
        per = d_tiles // ranks
        target = lax.rem(rank + 1 + i // per, ranks)
        return column_copy(wd_ref, target * share + (i % per) * d_width, d_width, first_d + i)

    def out_start(i):
        slot = slot_of(first_o + i)
        for s in range(o_stack):
            pltpu.make_async_copy(
                wo_ref.at[:, pl.ds(i * o_cols + s * TILE, TILE)],
                ring.at[slot, pl.ds(s * own_rows, own_rows), :],
                ring_sem.at[slot],
            ).start()

    def out_wait(i):
        slot = slot_of(first_o + i)
        pltpu.make_async_copy(ring.at[slot], ring.at[slot], ring_sem.at[slot]).wait()

    def start_tile(tile):
        if tile >= last:
            return
        if tile < first_k:
            q_copy(tile).start()
        elif tile < first_v:
            k_copy(tile - first_k).start()
        elif tile < first_o:
            v_copy(tile - first_v).start()
        elif tile < first_g:
            out_start(tile - first_o)
        elif tile < first_d:
            gate_copy((tile - first_g) // 2, (tile - first_g) % 2).start()
        else:
            down_copy(tile - first_d).start()

    own_columns = pl.ds(pl.multiple_of(rank * share, share), share)
    own_load = pltpu.make_async_copy(tokens_ref, tok_all.at[:, own_columns], tok_sem)
    own_load.start()
    for tile in range(first_o):
        start_tile(tile)

    x_to = me + 1 - 2 * lax.rem(me, 2)
    y_to = me + 2 - 4 * lax.rem(lax.div(me, 2), 2)
    hops = ((x_to, y_to), (y_to, x_to))

    barrier = pltpu.get_barrier_semaphore()
    for peer in peers:
        pl.semaphore_signal(barrier, inc=1, device_id={"tp": peer}, device_id_type=MESH)
    near = [x_to, y_to] + [xor(me, 4 * j, bits) for j in range(1, planes)]
    for other in near:
        pl.semaphore_signal(barrier, inc=1, device_id={"dp": other}, device_id_type=MESH)
    pl.semaphore_wait(barrier, len(near) + len(peers))

    def to_peer(source, target, send_sem, recv_sem, peer):
        return pltpu.make_async_remote_copy(
            src_ref=source,
            dst_ref=target,
            send_sem=send_sem,
            recv_sem=recv_sem,
            device_id={"tp": peer},
            device_id_type=MESH,
        )

    sends = []
    for t, peer in enumerate(peers):
        copy = to_peer(
            tokens_ref, tok_all.at[:, own_columns], tok_send.at[t], tok_recv.at[t], peer
        )
        copy.start()
        sends.append(copy)
    kv_load = pltpu.make_async_copy(kv_ref, kv_buf, kv_sem)
    kv_load.start()
    own_load.wait()
    for t in range(ranks - 1):
        came = lax.rem(rank + 2 * ranks - 1 - t, ranks)
        landed = tok_all.at[:, pl.ds(pl.multiple_of(came * share, share), share)]
        pltpu.make_async_copy(landed, landed, tok_recv.at[t]).wait()

    def normalize(gain):
        squares = jnp.zeros((rows, 1), jnp.float32)
        for start in range(0, model, share):
            piece = tok_all[:, start : start + share].astype(jnp.float32)
            squares = squares + jnp.sum(piece * piece, axis=-1, keepdims=True)
        factor = lax.rsqrt(squares / model + EPS)
        for start in range(0, model, share):
            piece = tok_all[:, start : start + share].astype(jnp.float32)
            normed[:, start : start + share] = (
                piece * factor * gain[:, start : start + share]
            ).astype(jnp.bfloat16)

    normalize(gain_ref)

    def rope(values):
        return values * cos_ref[...] + pltpu.roll(values, width // 2, 1) * sin_ref[...]

    def send_query(piece, block, target, key):
        cut = pl.ds(piece * shared, shared)
        pltpu.make_async_remote_copy(
            src_ref=q_all.at[block, cut],
            dst_ref=q_all.at[block, cut],
            send_sem=q_send.at[piece, key],
            recv_sem=q_recv.at[piece, key],
            device_id={"dp": target},
            device_id_type=MESH,
        ).start()

    def block_of(piece, key):
        if piece % 2:
            low = lax.rem(key, 4)
            key = key - low + lax.div(low, 2) + 2 * lax.rem(low, 2)
        return xor(me, key, bits)

    tiles_each = q_tiles // kv_heads
    per_tile = q_width // width
    for piece in range(kv_heads):

        def project(t, carry, piece=piece):
            tile = piece * tiles_each + t
            q_copy(tile).wait()
            values = jnp.dot(
                normed[...],
                ring[slot_of(tile), :, 0:q_width],
                preferred_element_type=jnp.float32,
            )
            for h in range(per_tile):
                q_all[me, tile * per_tile + h] = rope(
                    values[:, h * width : (h + 1) * width]
                ).astype(jnp.bfloat16)
            return carry

        lax.fori_loop(0, tiles_each, project, 0)
        for link in range(2):
            send_query(piece, me, hops[piece % 2][link], 1 + link)
        for j in range(1, planes):
            send_query(piece, me, xor(me, 4 * j, bits), 4 * j)

    for i in range(k_tiles):
        k_copy(i).wait()
        values = jnp.dot(
            normed[...], ring[first_k + i, :, 0:k_width], preferred_element_type=jnp.float32
        )
        for h in range(k_width // width):
            new_k[i * (k_width // width) + h] = rope(
                values[:, h * width : (h + 1) * width]
            ).astype(jnp.bfloat16)
    for i in range(k_tiles):
        v_copy(i).wait()
        values = jnp.dot(
            normed[...], ring[first_v + i, :, 0:k_width], preferred_element_type=jnp.float32
        )
        for h in range(k_width // width):
            new_v[i * (k_width // width) + h] = values[:, h * width : (h + 1) * width].astype(
                jnp.bfloat16
            )
    for tile in range(first_o, slots + first_o):
        start_tile(tile)
    kv_load.wait()

    scale = LOG2E / math.sqrt(width)

    def attend(keys, values, ok, block, piece):
        queries = q_all[block, piece * shared : (piece + 1) * shared]
        queries = queries.reshape(shared * rows, width)
        scores = lax.dot_general(
            keys, queries, (((1,), (1,)), ((), ())), preferred_element_type=jnp.float32
        )
        scores = jnp.where(ok, scores * scale, NEG)
        highest = jnp.max(scores, axis=0, keepdims=True)
        expo = jnp.exp2(scores - highest)
        count = jnp.sum(expo, axis=0, keepdims=True)
        summed = lax.dot_general(
            values,
            expo.astype(jnp.bfloat16),
            (((0,), (0,)), ((), ())),
            preferred_element_type=jnp.float32,
        )
        return highest, count, summed

    def keep(found, part_to, stat_to):
        highest, count, summed = found
        for j in range(shared):
            lanes = slice(j * rows, (j + 1) * rows)
            part_to[j] = summed[:, lanes].astype(jnp.bfloat16)
            stat_to[j : j + 1] = highest[:, lanes]
            stat_to[shared + j : shared + j + 1] = count[:, lanes]

    key_row = lax.broadcasted_iota(jnp.int32, (rows, shared * rows), 0)
    token = lax.rem(lax.broadcasted_iota(jnp.int32, (rows, shared * rows), 1), rows)
    for piece in range(kv_heads):
        keep(
            attend(new_k[piece], new_v[piece], key_row <= token, me, piece),
            box.at[piece, 0],
            stat_box.at[piece, 0],
        )

    def send_part(piece, block, target, key):
        for source, target_box, out_sem, in_sem in (
            (part, box, part_send, part_recv),
            (stat, stat_box, stat_send, stat_recv),
        ):
            pltpu.make_async_remote_copy(
                src_ref=source.at[block, piece],
                dst_ref=target_box.at[piece, key],
                send_sem=out_sem.at[piece, key],
                recv_sem=in_sem.at[piece, key],
                device_id={"dp": target},
                device_id_type=MESH,
            ).start()

    def landed_part(piece, key):
        for target_box, in_sem in ((box, part_recv), (stat_box, stat_recv)):
            landed = target_box.at[piece, key]
            pltpu.make_async_copy(landed, landed, in_sem.at[piece, key]).wait()

    def landed_query(piece, key, block):
        landed = q_all.at[block, pl.ds(piece * shared, shared)]
        pltpu.make_async_copy(landed, landed, q_recv.at[piece, key]).wait()

    row = lax.broadcasted_iota(jnp.int32, (page, 1), 0)

    def one_key(key, carry):
        turn = lax.rem(key, 4)
        for piece in range(kv_heads):
            block = block_of(piece, key)
            near_to, far_to = hops[piece % 2]

            @pl.when(key > 0)
            def _():
                landed_query(piece, key, block)

                @pl.when(turn == 0)
                def _():
                    send_query(piece, block, near_to, key + 1)

                @pl.when(turn < 2)
                def _():
                    send_query(piece, block, far_to, key + 2)

            pages = [slot_ref[block, k] for k in range(per_owner)]
            ok = jnp.concatenate([row < valid_ref[block, k] for k in range(per_owner)], axis=0)
            keys = jnp.concatenate([kv_buf[p, 0, piece] for p in pages], axis=0)
            values = jnp.concatenate([kv_buf[p, 1, piece] for p in pages], axis=0)
            keep(
                attend(keys, values, ok, block, piece),
                part.at[block, piece],
                stat.at[block, piece],
            )

            @pl.when(turn >= 2)
            def _():
                send_part(piece, block, far_to, key)

        return carry

    lax.fori_loop(0, groups, one_key, 0)

    def merge_into(piece, block, key):
        merged, mine, other = merge_stats(stat[block, piece], stat_box[piece, key])
        for j in range(shared):
            part[block, piece, j] = (
                part[block, piece, j].astype(jnp.float32) * mine[j : j + 1]
                + box[piece, key, j].astype(jnp.float32) * other[j : j + 1]
            ).astype(jnp.bfloat16)
        stat[block, piece] = merged

    def first_merges(index, carry):
        base = 4 * (planes - 1 - index)
        for turn in (1, 0):
            for piece in range(kv_heads):
                block = block_of(piece, base + turn)
                landed_part(piece, base + turn + 2)
                merge_into(piece, block, base + turn + 2)
                if turn:
                    send_part(piece, block, hops[piece % 2][0], base + 1)
        return carry

    lax.fori_loop(0, planes, first_merges, 0)

    def second_merges(index, carry):
        base = 4 * (planes - 1 - index)
        for piece in range(kv_heads):
            block = block_of(piece, base)
            landed_part(piece, base + 1)
            merge_into(piece, block, base + 1)

            @pl.when(base > 0)
            def _():
                send_part(piece, block, block, base)

        return carry

    lax.fori_loop(0, planes, second_merges, 0)

    for piece in range(kv_heads):

        def home_merge(j, carry, piece=piece):
            @pl.when(j > 0)
            def _():
                landed_part(piece, 4 * j)

            merged, mine, other = merge_stats(carry[0], stat_box[piece, 4 * j])
            sums = tuple(
                carry[1 + h] * mine[h : h + 1]
                + box[piece, 4 * j, h].astype(jnp.float32) * other[h : h + 1]
                for h in range(shared)
            )
            return (merged,) + sums

        start = (stat[me, piece],) + tuple(
            part[me, piece, h].astype(jnp.float32) for h in range(shared)
        )
        done = lax.fori_loop(0, planes, home_merge, start)
        for h in range(shared):
            lanes = slice((piece * shared + h) * width, (piece * shared + h + 1) * width)
            total = done[0][shared + h : shared + h + 1]
            context_ref[:, lanes] = (done[1 + h] / total).T.astype(jnp.bfloat16)

    for i in range(o_tiles):
        out_wait(i)
        for s in range(o_stack):
            start = i * o_cols + s * TILE
            attn_all[rank, :, start : start + TILE] = jnp.dot(
                context_ref[...],
                ring[slot_of(first_o + i), s * own_rows : (s + 1) * own_rows, :],
                preferred_element_type=jnp.float32,
            ).astype(jnp.bfloat16)
        start_tile(first_o + i + slots)
        for t, peer in enumerate(peers):
            ready = attn_all.at[rank, :, pl.ds(i * o_cols, o_cols)]
            copy = to_peer(ready, ready, attn_send.at[t, i], attn_recv.at[t, i], peer)
            copy.start()
            sends.append(copy)
    for i in range(o_tiles):
        columns = pl.ds(i * o_cols, o_cols)
        for t in range(ranks - 1):
            landed = attn_all.at[lax.rem(rank + 2 * ranks - 1 - t, ranks), :, columns]
            pltpu.make_async_copy(landed, landed, attn_recv.at[t, i]).wait()
        attn_sum = attn_all[0, :, columns].astype(jnp.float32)
        for r in range(1, ranks):
            attn_sum = attn_sum + attn_all[r, :, columns].astype(jnp.float32)
        tok_all[:, columns] = (tok_all[:, columns].astype(jnp.float32) + attn_sum).astype(
            jnp.bfloat16
        )

    normalize(mlp_gain_ref)

    def gate_step(i, carry):
        gate_copy(i, 0).wait()
        gate = jnp.dot(
            normed[...],
            ring[slot_of(first_g + 2 * i), :, 0:g_width],
            preferred_element_type=jnp.float32,
        )
        gate_copy(i, 1).wait()
        up = jnp.dot(
            normed[...],
            ring[slot_of(first_g + 2 * i + 1), :, 0:g_width],
            preferred_element_type=jnp.float32,
        )
        columns = pl.ds(pl.multiple_of(i * g_width, g_width), g_width)
        hidden[:, columns] = (gate / (1.0 + jnp.exp(-gate)) * up).astype(jnp.bfloat16)
        later = i + slots // 2

        @pl.when(later < g_tiles)
        def _():
            gate_copy(later, 0).start()
            gate_copy(later, 1).start()

        for which in range(2):
            down = 2 * (later - g_tiles) + which

            @pl.when((later >= g_tiles) & (down < d_tiles))
            def _():
                down_copy(down).start()

        return carry

    lax.fori_loop(0, g_tiles, gate_step, 0)

    per_target = d_tiles // ranks
    for t in range(ranks):

        def down_step(index, carry, t=t):
            i = index + t * per_target
            down_copy(i).wait()
            columns = pl.ds(pl.multiple_of(index * d_width, d_width), d_width)
            mlp_part[t, :, columns] = jnp.dot(
                hidden[...],
                ring[slot_of(first_d + i), 0:units, 0:d_width],
                preferred_element_type=jnp.float32,
            ).astype(jnp.bfloat16)

            @pl.when(i + slots < d_tiles)
            def _():
                down_copy(i + slots).start()

            return carry

        lax.fori_loop(0, per_target, down_step, 0)
        if t < ranks - 1:
            copy = to_peer(
                mlp_part.at[t], mlp_box.at[t], mlp_send.at[t], mlp_recv.at[t], peers[t]
            )
            copy.start()
            sends.append(copy)
    mlp_sum = mlp_part[ranks - 1].astype(jnp.float32)
    for t in range(ranks - 1):
        pltpu.make_async_copy(mlp_box.at[t], mlp_box.at[t], mlp_recv.at[t]).wait()
        mlp_sum = mlp_sum + mlp_box[t].astype(jnp.float32)
    layer_ref[...] = (tok_all[:, own_columns].astype(jnp.float32) + mlp_sum).astype(jnp.bfloat16)

    for copy in sends:
        copy.wait_send()

    def settle(key, carry):
        for piece in range(kv_heads):
            sent = q_all.at[0, pl.ds(piece * shared, shared)]
            pltpu.make_async_copy(sent, sent, q_send.at[piece, key]).wait()
            for source, out_sem in ((part, part_send), (stat, stat_send)):
                sent = source.at[0, piece]
                pltpu.make_async_copy(sent, sent, out_sem.at[piece, key]).wait()
        return carry

    lax.fori_loop(1, groups, settle, 0)


def layer(groups, ranks, per_owner, tables, gains, tokens, weights, kv_pool):
    slot_pick, valid, cosine, sine = tables
    rows, share = tokens.shape
    model = share * ranks
    _, _, kv_heads, page, width = kv_pool.shape
    heads = weights[0].shape[1] // width
    units = weights[4].shape[1]
    shared = heads // kv_heads
    bf16 = jnp.bfloat16
    dma = pltpu.SemaphoreType.DMA
    vmem = pl.BlockSpec(memory_space=VMEM)
    smem = pl.BlockSpec(memory_space=pltpu.SMEM)
    hbm = pl.BlockSpec(memory_space=pl.ANY)
    buffers = [
        (kv_pool.shape, bf16),
        ((rows, model), bf16),
        ((rows, model), bf16),
        ((groups, heads, rows, width), bf16),
        ((kv_heads, rows, width), bf16),
        ((kv_heads, rows, width), bf16),
        ((groups, kv_heads, shared, width, rows), bf16),
        ((groups, kv_heads, 2 * shared, rows), jnp.float32),
        ((kv_heads, groups, shared, width, rows), bf16),
        ((kv_heads, groups, 2 * shared, rows), jnp.float32),
        ((ranks, rows, model), bf16),
        ((rows, units), bf16),
        ((ranks, rows, share), bf16),
        ((ranks, rows, share), bf16),
    ]
    used = sum(math.prod(shape) * jnp.dtype(kind).itemsize for shape, kind in buffers)
    used += 2 * rows * (heads * width + share) + 8 * rows * width + 64 * model + 2_500_000
    slots = (VMEM_BUDGET - used) // (2 * model * TILE) // 2 * 2
    return pl.pallas_call(
        functools.partial(layer_kernel, (groups, ranks, kv_heads, per_owner)),
        out_shape=(
            jax.ShapeDtypeStruct((rows, heads * width), bf16),
            jax.ShapeDtypeStruct((rows, share), bf16),
        ),
        in_specs=[smem, smem, vmem, vmem, vmem, vmem] + [hbm] * 9,
        out_specs=(vmem, vmem),
        scratch_shapes=[VMEM((slots, model, TILE), bf16)]
        + [VMEM(shape, kind) for shape, kind in buffers]
        + [
            dma((slots,)),
            dma,
            dma,
            dma((ranks,)),
            dma((ranks,)),
            dma((kv_heads, groups)),
            dma((kv_heads, groups)),
            dma((kv_heads, groups)),
            dma((kv_heads, groups)),
            dma((kv_heads, groups)),
            dma((kv_heads, groups)),
            dma((ranks, 8)),
            dma((ranks, 8)),
            dma((ranks,)),
            dma((ranks,)),
        ],
        compiler_params=pltpu.CompilerParams(
            collective_id=0, has_side_effects=True, vmem_limit_bytes=67_000_000
        ),
        name="layer",
    )(slot_pick, valid, cosine, sine, *gains, tokens, *weights, kv_pool)


def shards(
    tokens,
    norm_gain,
    w_query,
    w_key,
    w_value,
    w_out,
    mlp_gain,
    w_gate,
    w_up,
    w_down,
    kv_pool,
    prefix_len,
    page_owner,
    page_slot,
    serving,
):
    groups = lax.axis_size("dp")
    device = lax.axis_index("dp")
    rows = tokens.shape[0]
    pages_max = page_owner.shape[1]
    per_owner = (pages_max + groups - 1) // groups
    page_len = kv_pool.shape[3]
    width = kv_pool.shape[4]
    ids = jnp.arange(groups, dtype=jnp.int32)
    served = serving[:, None] == ids[None, :]
    lengths = jnp.sum(jnp.where(served, prefix_len[None, :], 0), axis=1)
    length = jnp.sum(jnp.where(ids == device, lengths, 0))
    half = jnp.arange(width // 2, dtype=jnp.float32)
    inverse = jnp.power(jnp.float32(THETA), -2.0 * half / width)
    positions = length + jnp.arange(rows, dtype=jnp.int32)
    angles = positions.astype(jnp.float32)[:, None] * inverse[None, :]
    cosine = jnp.cos(angles)
    sine = jnp.sin(angles)
    cosine = jnp.concatenate([cosine, cosine], axis=1)
    sine = jnp.concatenate([-sine, sine], axis=1)
    owners = jnp.sum(jnp.where(served[:, :, None], page_owner[None], 0), axis=1)
    held = jnp.sum(jnp.where(served[:, :, None], page_slot[None], 0), axis=1)
    pages = jnp.arange(pages_max, dtype=jnp.int32)
    owned = owners == device
    rank = jnp.sum(
        jnp.where(pages[None, :, None] > pages[None, None, :], owned[:, None, :], False).astype(
            jnp.int32
        ),
        axis=2,
    )
    left = jnp.clip(lengths[:, None] - pages[None, :] * page_len, 0, page_len)
    choose = jnp.arange(per_owner, dtype=jnp.int32)
    picked = owned[:, None, :] & (rank[:, None, :] == choose[None, :, None])
    slot_pick = jnp.sum(jnp.where(picked, held[:, None, :], 0), axis=2)
    valid = jnp.sum(jnp.where(picked, left[:, None, :], 0), axis=2)
    return layer(
        groups,
        lax.axis_size("tp"),
        per_owner,
        (slot_pick, valid, cosine, sine),
        (norm_gain[None, :], mlp_gain[None, :]),
        tokens,
        (w_query, w_key, w_value, w_out, w_gate, w_up, w_down),
        kv_pool,
    )


def solution(mesh):
    in_specs = (
        P("dp", "tp"),
        P(),
        P(None, "tp"),
        P(None, "tp"),
        P(None, "tp"),
        P("tp", None),
        P(),
        P(None, "tp"),
        P(None, "tp"),
        P("tp", None),
        P("dp", None, "tp", None, None),
        P(),
        P(),
        P(),
        P(),
    )
    out_specs = (P("dp", "tp"), P("dp", "tp"))
    return jax.shard_map(shards, mesh=mesh, in_specs=in_specs, out_specs=out_specs, check_vma=False)
```

```python
import functools
import math

import jax
import jax.numpy as jnp
import numpy as np
from jax import lax
from jax.experimental import pallas as pl
from jax.experimental.pallas import tpu as pltpu
from jax.sharding import PartitionSpec as P

EPS = 1e-05
THETA = 500000.0
NEG = -1e30
LOG2E = 1.4426950408889634
MESH = pl.DeviceIdType.MESH
VMEM = pltpu.VMEM
VMEM_BUDGET = 66_800_000
TILE = 256


def xor(a, b, bits):
    out = 0
    for bit in range(bits):
        unit = 1 << bit
        out = out + lax.rem(lax.div(a, unit) + lax.div(b, unit), 2) * unit
    return out


TUNED = (
    "C0", "I0.12", "I0.4", "I0.1", "C1", "I1.12", "I1.2", "I1.1", "I0.2", "I1.4", "F0.1",
    "F1.1", "F0.12", "I1.8", "C2", "F0.2", "F0.4", "F1.12", "I0.8", "F1.4", "A1", "F0.13",
    "F1.13", "F1.8", "F0.6", "F0.14", "F0.15", "F1.15", "F0.8", "F1.2", "A15", "R0.15", "F1.6",
    "F1.9", "F1.14", "F0.5", "A12", "F1.5", "F0.9", "A13", "F1.10", "A4", "F1.11", "F0.10",
    "R1.15", "M0.13", "A14", "A10", "R1.14", "R0.10", "F0.7", "F1.7", "A6", "A7", "M1.13",
    "F0.11", "R0.14", "A5", "R1.7", "A9", "A11", "R1.11", "M1.12", "A2", "R0.11", "R1.10",
    "R0.7", "N1.3", "M1.5", "M1.9", "M0.12", "F0.3", "R0.6", "N0.3", "M0.9", "F1.3", "A8", "A3",
    "R0.3", "R1.6", "R1.3", "M1.8", "M0.8", "N0.2", "R1.2", "M0.5", "M1.4", "R0.2", "A0",
    "N1.1", "N1.2", "M0.1", "M1.0", "M0.4", "M1.1", "N0.1", "N1.0", "M0.0", "N0.0",
)


def schedule(planes):
    if planes == 4:
        return [(word[0], [int(part) for part in word[1:].split(".")]) for word in TUNED]
    tasks = []
    for piece in range(2):
        tasks.append(("C", [piece]))
        tasks += [("I", [piece, key]) for key in (1, 2)]
        tasks += [("I", [piece, 4 * j]) for j in range(1, planes)]
    tasks.append(("C", [2]))
    for key in range(4 * planes):
        tasks += [("F", [piece, key]) for piece in range(2) if key]
        tasks.append(("A", [key]))
        tasks += [("R", [piece, key]) for piece in range(2) if key % 4 >= 2]
    for j in reversed(range(planes)):
        tasks += [("M", [piece, 4 * j + turn]) for turn in (1, 0) for piece in range(2)]
    for j in reversed(range(planes)):
        tasks += [("N", [piece, j]) for piece in range(2)]
    return tasks


def flipped(me, mask):
    out = me
    bit = 1
    while bit <= mask:
        if mask & bit:
            out = out + (1 - 2 * lax.rem(lax.div(me, bit), 2)) * bit
        bit *= 2
    return out


def merge_stats(left, right):
    shared = left.shape[0] // 2
    top = jnp.maximum(left[:shared], right[:shared])
    factor_left = jnp.exp2(left[:shared] - top)
    factor_right = jnp.exp2(right[:shared] - top)
    count = left[shared:] * factor_left + right[shared:] * factor_right
    return jnp.concatenate([top, count], axis=0), factor_left, factor_right


def layer_kernel(
    plan,
    length_ref,
    serving_ref,
    owner_ref,
    page_slot_ref,
    inverse_ref,
    norm_gain_ref,
    mlp_norm_gain_ref,
    tokens_ref,
    wq_ref,
    wk_ref,
    wv_ref,
    wo_ref,
    wg_ref,
    wu_ref,
    wd_ref,
    kv_ref,
    context_out,
    layer_out,
    ring,
    kv_buf,
    tok_all,
    normed,
    q_all,
    new_k,
    new_v,
    part,
    stat,
    box,
    stat_box,
    attn_all,
    hidden,
    mlp_part,
    mlp_box,
    context_ref,
    layer_ref,
    cos_ref,
    sin_ref,
    inverse_buf,
    gain_ref,
    mlp_gain_ref,
    owner_buf,
    page_slot_buf,
    owner_rows,
    slot_rows,
    length_rows,
    picks,
    picked,
    small_sem,
    picks_sem,
    out_sem,
    ring_sem,
    kv_sem,
    tok_sem,
    tok_send,
    tok_recv,
    q_send,
    q_recv,
    part_send,
    part_recv,
    stat_send,
    stat_recv,
    attn_send,
    attn_recv,
    mlp_send,
    mlp_recv,
):
    groups, ranks, kv_heads, per_owner = plan
    me = lax.axis_index("dp")
    rank = lax.axis_index("tp")
    bits = groups.bit_length() - 1
    planes = groups // 4
    rows, model = normed.shape
    share = tokens_ref.shape[1]
    width = q_all.shape[3]
    heads = q_all.shape[1]
    shared = heads // kv_heads
    page = kv_ref.shape[3]
    slots = ring.shape[0]
    units = wd_ref.shape[0]
    own_rows = wo_ref.shape[0]
    peers = [lax.rem(rank + 1 + t, ranks) for t in range(ranks - 1)]

    def slabs(total):
        step = math.gcd(total, TILE)
        return step, total // step

    q_width, q_tiles = slabs(wq_ref.shape[1])
    k_width, k_tiles = slabs(wk_ref.shape[1])
    g_width, g_tiles = slabs(units)
    d_width, d_tiles = slabs(share)
    d_tiles = d_tiles * ranks
    o_stack = model // own_rows
    o_cols = o_stack * TILE
    o_tiles = model // o_cols
    first_k = q_tiles
    first_v = first_k + k_tiles
    first_o = first_v + k_tiles
    first_g = first_o + o_tiles
    first_d = first_g + 2 * g_tiles
    last = first_d + d_tiles

    def slot_of(tile):
        return tile % slots if isinstance(tile, int) else lax.rem(tile, slots)

    def column_copy(source, start, step, tile):
        slot = slot_of(tile)
        count = source.shape[0]
        columns = pl.ds(pl.multiple_of(start, step), step)
        return pltpu.make_async_copy(
            source.at[:, columns],
            ring.at[slot, pl.ds(0, count), pl.ds(0, step)],
            ring_sem.at[slot],
        )

    def q_copy(i):
        return column_copy(wq_ref, i * q_width, q_width, i)

    def k_copy(i):
        return column_copy(wk_ref, i * k_width, k_width, first_k + i)

    def v_copy(i):
        return column_copy(wv_ref, i * k_width, k_width, first_v + i)

    def gate_copy(i, which):
        return column_copy((wg_ref, wu_ref)[which], i * g_width, g_width, first_g + 2 * i + which)

    def down_copy(i):
        per = d_tiles // ranks
        target = lax.rem(rank + 1 + i // per, ranks)
        return column_copy(wd_ref, target * share + (i % per) * d_width, d_width, first_d + i)

    def out_start(i):
        slot = slot_of(first_o + i)
        for s in range(o_stack):
            pltpu.make_async_copy(
                wo_ref.at[:, pl.ds(i * o_cols + s * TILE, TILE)],
                ring.at[slot, pl.ds(s * own_rows, own_rows), :],
                ring_sem.at[slot],
            ).start()

    def out_wait(i):
        slot = slot_of(first_o + i)
        pltpu.make_async_copy(ring.at[slot], ring.at[slot], ring_sem.at[slot]).wait()

    def start_tile(tile):
        if tile >= last:
            return
        if tile < first_k:
            q_copy(tile).start()
        elif tile < first_v:
            k_copy(tile - first_k).start()
        elif tile < first_o:
            v_copy(tile - first_v).start()
        elif tile < first_g:
            out_start(tile - first_o)
        elif tile < first_d:
            gate_copy((tile - first_g) // 2, (tile - first_g) % 2).start()
        else:
            down_copy(tile - first_d).start()

    own_columns = pl.ds(pl.multiple_of(rank * share, share), share)
    own_load = pltpu.make_async_copy(tokens_ref, tok_all.at[:, own_columns], tok_sem)
    own_load.start()
    small = [
        pltpu.make_async_copy(source, target, small_sem.at[i])
        for i, (source, target) in enumerate(
            (
                (norm_gain_ref, gain_ref),
                (inverse_ref, inverse_buf),
                (owner_ref, owner_buf),
                (page_slot_ref, page_slot_buf),
                (mlp_norm_gain_ref, mlp_gain_ref),
            )
        )
    ]
    for copy in small:
        copy.start()
    for tile in range(first_o):
        start_tile(tile)

    x_to = me + 1 - 2 * lax.rem(me, 2)
    y_to = me + 2 - 4 * lax.rem(lax.div(me, 2), 2)
    hops = ((x_to, y_to), (y_to, x_to))

    barrier = pltpu.get_barrier_semaphore()
    for peer in peers:
        pl.semaphore_signal(barrier, inc=1, device_id={"tp": peer}, device_id_type=MESH)
    near = [x_to, y_to] + [xor(me, 4 * j, bits) for j in range(1, planes)]
    for other in near:
        pl.semaphore_signal(barrier, inc=1, device_id={"dp": other}, device_id_type=MESH)
    pl.semaphore_wait(barrier, len(near) + len(peers))

    def to_peer(source, target, send_sem, recv_sem, peer):
        return pltpu.make_async_remote_copy(
            src_ref=source,
            dst_ref=target,
            send_sem=send_sem,
            recv_sem=recv_sem,
            device_id={"tp": peer},
            device_id_type=MESH,
        )

    sends = []
    for t, peer in enumerate(peers):
        copy = to_peer(
            tokens_ref, tok_all.at[:, own_columns], tok_send.at[t], tok_recv.at[t], peer
        )
        copy.start()
        sends.append(copy)
    kv_load = pltpu.make_async_copy(kv_ref, kv_buf, kv_sem)
    kv_load.start()
    for copy in small:
        copy.wait()

    length = length_ref[serving_ref[me]]
    position = length + lax.broadcasted_iota(jnp.int32, (rows, width), 0)
    angles = position.astype(jnp.float32) * inverse_buf[...]
    lane = lax.broadcasted_iota(jnp.int32, (rows, width), 1)
    cos_ref[...] = jnp.cos(angles)
    sine = jnp.sin(angles)
    sin_ref[...] = jnp.where(lane < width // 2, -sine, sine)

    pages_max = owner_buf.shape[1]
    span = owner_rows.shape[1]

    def group_row(group, carry):
        request = serving_ref[group]
        here = pl.ds(group, 1)
        owner_rows[here, 0:pages_max] = owner_buf[pl.ds(request, 1), :]
        slot_rows[here, 0:pages_max] = page_slot_buf[pl.ds(request, 1), :]
        length_rows[here, :] = jnp.full((1, span), length_ref[request], jnp.int32)
        return carry

    lax.fori_loop(0, groups, group_row, 0)
    lane = lax.broadcasted_iota(jnp.int32, (groups, span), 1)
    owned = ((owner_rows[...] == me) & (lane < pages_max)).astype(jnp.int32)
    before = owned
    shift = 1
    while shift < span:
        before = before + jnp.where(lane >= shift, pltpu.roll(before, shift, 1), 0)
        shift *= 2
    before = before - owned
    left = jnp.clip(length_rows[...] - lane * page, 0, page)
    table = jnp.zeros((groups, span), jnp.int32)
    for k in range(per_owner):
        chosen = (owned > 0) & (before == k)
        for at, source in ((k, slot_rows[...]), (per_owner + k, left)):
            value = jnp.sum(jnp.where(chosen, source, 0), axis=1, keepdims=True)
            table = table + jnp.where(lane == at, value, 0)
    picks[...] = table
    picks_copy = pltpu.make_async_copy(picks, picked, picks_sem)
    picks_copy.start()

    own_load.wait()
    for t in range(ranks - 1):
        came = lax.rem(rank + 2 * ranks - 1 - t, ranks)
        landed = tok_all.at[:, pl.ds(pl.multiple_of(came * share, share), share)]
        pltpu.make_async_copy(landed, landed, tok_recv.at[t]).wait()

    def normalize(gain):
        squares = jnp.zeros((rows, 1), jnp.float32)
        for start in range(0, model, share):
            piece = tok_all[:, start : start + share].astype(jnp.float32)
            squares = squares + jnp.sum(piece * piece, axis=-1, keepdims=True)
        factor = lax.rsqrt(squares / model + EPS)
        for start in range(0, model, share):
            piece = tok_all[:, start : start + share].astype(jnp.float32)
            normed[:, start : start + share] = (
                piece * factor * gain[:, start : start + share]
            ).astype(jnp.bfloat16)

    normalize(gain_ref)

    def rope(values):
        return values * cos_ref[...] + pltpu.roll(values, width // 2, 1) * sin_ref[...]

    def send_query(piece, block, target, key):
        cut = pl.ds(piece * shared, shared)
        pltpu.make_async_remote_copy(
            src_ref=q_all.at[block, cut],
            dst_ref=q_all.at[block, cut],
            send_sem=q_send.at[piece, key],
            recv_sem=q_recv.at[piece, key],
            device_id={"dp": target},
            device_id_type=MESH,
        ).start()

    def block_of(piece, key):
        if piece % 2:
            low = lax.rem(key, 4)
            key = key - low + lax.div(low, 2) + 2 * lax.rem(low, 2)
        return xor(me, key, bits)

    def block_at(piece, key):
        low = key % 4
        if piece % 2:
            low = low // 2 + 2 * (low % 2)
        return flipped(me, key - key % 4 + low)

    tiles_each = q_tiles // kv_heads
    per_tile = q_width // width

    def project(piece):
        tiles = [piece * tiles_each + t for t in range(tiles_each)]
        for tile in tiles:
            q_copy(tile).wait()
        for tile in tiles:
            values = jnp.dot(
                normed[...], ring[tile, :, 0:q_width], preferred_element_type=jnp.float32
            )
            for h in range(per_tile):
                q_all[me, tile * per_tile + h] = rope(
                    values[:, h * width : (h + 1) * width]
                ).astype(jnp.bfloat16)

    def send_own(piece, key):
        target = hops[piece % 2][key - 1] if key < 4 else flipped(me, key)
        send_query(piece, me, target, key)

    def forward(piece, key):
        block = block_at(piece, key)
        landed = q_all.at[block, pl.ds(piece * shared, shared)]
        pltpu.make_async_copy(landed, landed, q_recv.at[piece, key]).wait()
        if key % 4 == 0:
            send_query(piece, block, hops[piece % 2][0], key + 1)
        if key % 4 < 2:
            send_query(piece, block, hops[piece % 2][1], key + 2)

    tasks = [
        (kind, spec)
        for kind, spec in schedule(planes)
        if kind in "CA" or spec[0] < kv_heads
    ]
    marks = [tasks.index(("C", [at])) for at in range(3)]
    for at in range(2):
        if at < kv_heads:
            project(at)
        for kind, spec in tasks[marks[at] + 1 : marks[at + 1]]:
            (send_own if kind == "I" else forward)(*spec)
    tasks = tasks[marks[2] + 1 :]

    for i in range(k_tiles):
        k_copy(i).wait()
        v_copy(i).wait()
    per_tile = k_width // width
    for i in range(k_tiles):
        for first, store, turn in ((first_k, new_k, rope), (first_v, new_v, lambda v: v)):
            values = jnp.dot(
                normed[...], ring[first + i, :, 0:k_width], preferred_element_type=jnp.float32
            )
            for h in range(per_tile):
                store[i * per_tile + h] = turn(values[:, h * width : (h + 1) * width]).astype(
                    jnp.bfloat16
                )
    for tile in range(first_o, slots + first_o):
        start_tile(tile)
    kv_load.wait()
    picks_copy.wait()

    scale = LOG2E / math.sqrt(width)

    def attend(keys, values, ok, block, piece):
        queries = q_all[block, piece * shared : (piece + 1) * shared]
        queries = queries.reshape(shared * rows, width)
        scores = lax.dot_general(
            keys, queries, (((1,), (1,)), ((), ())), preferred_element_type=jnp.float32
        )
        scores = jnp.where(ok, scores * scale, NEG)
        highest = jnp.max(scores, axis=0, keepdims=True)
        expo = jnp.exp2(scores - highest)
        count = jnp.sum(expo, axis=0, keepdims=True)
        summed = lax.dot_general(
            values,
            expo.astype(jnp.bfloat16),
            (((0,), (0,)), ((), ())),
            preferred_element_type=jnp.float32,
        )
        return highest, count, summed

    def keep(found, part_to, stat_to):
        highest, count, summed = found
        for j in range(shared):
            lanes = slice(j * rows, (j + 1) * rows)
            part_to[j] = summed[:, lanes].astype(jnp.bfloat16)
            stat_to[j : j + 1] = highest[:, lanes]
            stat_to[shared + j : shared + j + 1] = count[:, lanes]

    key_row = lax.broadcasted_iota(jnp.int32, (rows, shared * rows), 0)
    token = lax.rem(lax.broadcasted_iota(jnp.int32, (rows, shared * rows), 1), rows)
    for piece in range(kv_heads):
        keep(
            attend(new_k[piece], new_v[piece], key_row <= token, me, piece),
            box.at[piece, 0],
            stat_box.at[piece, 0],
        )

    def send_part(piece, block, target, key):
        for source, target_box, out_sem, in_sem in (
            (part, box, part_send, part_recv),
            (stat, stat_box, stat_send, stat_recv),
        ):
            pltpu.make_async_remote_copy(
                src_ref=source.at[block, piece],
                dst_ref=target_box.at[piece, key],
                send_sem=out_sem.at[piece, key],
                recv_sem=in_sem.at[piece, key],
                device_id={"dp": target},
                device_id_type=MESH,
            ).start()

    def landed_part(piece, key):
        for target_box, in_sem in ((box, part_recv), (stat_box, stat_recv)):
            landed = target_box.at[piece, key]
            pltpu.make_async_copy(landed, landed, in_sem.at[piece, key]).wait()

    row = lax.broadcasted_iota(jnp.int32, (page, 1), 0)

    def merge_into(piece, block, key):
        merged, mine, other = merge_stats(stat[block, piece], stat_box[piece, key])
        for j in range(shared):
            part[block, piece, j] = (
                part[block, piece, j].astype(jnp.float32) * mine[j : j + 1]
                + box[piece, key, j].astype(jnp.float32) * other[j : j + 1]
            ).astype(jnp.bfloat16)
        stat[block, piece] = merged

    def run_task(kind, piece, key):
        near_to, far_to = hops[piece % 2]
        if kind == "I":
            send_own(piece, key)
            return
        if kind == "N":
            block = block_at(piece, 4 * key)
            landed_part(piece, 4 * key + 1)
            merge_into(piece, block, 4 * key + 1)
            if key:
                send_part(piece, block, block, 4 * key)
            return
        block = block_at(piece, key)
        if kind == "F":
            forward(piece, key)
        elif kind == "R":
            send_part(piece, block, far_to, key)
        elif kind == "M":
            landed_part(piece, key + 2)
            merge_into(piece, block, key + 2)
            if key % 4 == 1:
                send_part(piece, block, near_to, key)

    before_turn = [[]]
    order = []
    for kind, spec in tasks:
        if kind == "A":
            order.append(spec[0])
            before_turn.append([])
        else:
            before_turn[-1].append((kind, *spec))

    def one_turn(turn, carry):
        for at, todo in enumerate(before_turn[:-1]):
            if todo:

                @pl.when(turn == at)
                def _():
                    for task in todo:
                        run_task(*task)

        key = 0
        for at, value in enumerate(order):
            key = jnp.where(turn == at, value, key)
        for piece in range(kv_heads):
            block = block_of(piece, key)
            pages = [picked[block, k] for k in range(per_owner)]
            ok = jnp.concatenate(
                [row < picked[block, per_owner + k] for k in range(per_owner)], axis=0
            )
            keys = jnp.concatenate([kv_buf[p, 0, piece] for p in pages], axis=0)
            values = jnp.concatenate([kv_buf[p, 1, piece] for p in pages], axis=0)
            keep(
                attend(keys, values, ok, block, piece),
                part.at[block, piece],
                stat.at[block, piece],
            )
        return carry

    lax.fori_loop(0, groups, one_turn, 0)
    for task in before_turn[-1]:
        run_task(*task)

    for piece in range(kv_heads):

        def home_merge(j, carry, piece=piece):
            @pl.when(j > 0)
            def _():
                landed_part(piece, 4 * j)

            merged, mine, other = merge_stats(carry[0], stat_box[piece, 4 * j])
            sums = tuple(
                carry[1 + h] * mine[h : h + 1]
                + box[piece, 4 * j, h].astype(jnp.float32) * other[h : h + 1]
                for h in range(shared)
            )
            return (merged,) + sums

        start = (stat[me, piece],) + tuple(
            part[me, piece, h].astype(jnp.float32) for h in range(shared)
        )
        done = lax.fori_loop(0, planes, home_merge, start)
        for h in range(shared):
            lanes = slice((piece * shared + h) * width, (piece * shared + h + 1) * width)
            total = done[0][shared + h : shared + h + 1]
            context_ref[:, lanes] = (done[1 + h] / total).T.astype(jnp.bfloat16)

    context_copy = pltpu.make_async_copy(context_ref, context_out, out_sem.at[0])
    context_copy.start()
    for i in range(o_tiles):
        out_wait(i)
        for s in range(o_stack):
            start = i * o_cols + s * TILE
            attn_all[rank, :, start : start + TILE] = jnp.dot(
                context_ref[...],
                ring[slot_of(first_o + i), s * own_rows : (s + 1) * own_rows, :],
                preferred_element_type=jnp.float32,
            ).astype(jnp.bfloat16)
        start_tile(first_o + i + slots)
        for t, peer in enumerate(peers):
            ready = attn_all.at[rank, :, pl.ds(i * o_cols, o_cols)]
            copy = to_peer(ready, ready, attn_send.at[t, i], attn_recv.at[t, i], peer)
            copy.start()
            sends.append(copy)
    for i in range(o_tiles):
        columns = pl.ds(i * o_cols, o_cols)
        for t in range(ranks - 1):
            landed = attn_all.at[lax.rem(rank + 2 * ranks - 1 - t, ranks), :, columns]
            pltpu.make_async_copy(landed, landed, attn_recv.at[t, i]).wait()
        attn_sum = attn_all[0, :, columns].astype(jnp.float32)
        for r in range(1, ranks):
            attn_sum = attn_sum + attn_all[r, :, columns].astype(jnp.float32)
        tok_all[:, columns] = (tok_all[:, columns].astype(jnp.float32) + attn_sum).astype(
            jnp.bfloat16
        )

    normalize(mlp_gain_ref)

    pairs = math.gcd(g_tiles, 2)

    def gate_step(index, carry):
        mine = [index * pairs + u for u in range(pairs)]
        for i in mine:
            gate_copy(i, 0).wait()
            gate_copy(i, 1).wait()
        for i in mine:
            gate, up = [
                jnp.dot(
                    normed[...],
                    ring[slot_of(first_g + 2 * i + which), :, 0:g_width],
                    preferred_element_type=jnp.float32,
                )
                for which in range(2)
            ]
            columns = pl.ds(pl.multiple_of(i * g_width, g_width), g_width)
            hidden[:, columns] = (gate / (1.0 + jnp.exp(-gate)) * up).astype(jnp.bfloat16)
        for i in mine:
            later = i + slots // 2

            @pl.when(later < g_tiles)
            def _():
                gate_copy(later, 0).start()
                gate_copy(later, 1).start()

            for which in range(2):
                down = 2 * (later - g_tiles) + which

                @pl.when((later >= g_tiles) & (down < d_tiles))
                def _():
                    down_copy(down).start()

        return carry

    lax.fori_loop(0, g_tiles // pairs, gate_step, 0)

    per_target = d_tiles // ranks
    fours = math.gcd(per_target, 4)
    for t in range(ranks):

        def down_step(index, carry, t=t):
            mine = [index * fours + u for u in range(fours)]
            for at in mine:
                down_copy(at + t * per_target).wait()
            for at in mine:
                columns = pl.ds(pl.multiple_of(at * d_width, d_width), d_width)
                mlp_part[t, :, columns] = jnp.dot(
                    hidden[...],
                    ring[slot_of(first_d + at + t * per_target), 0:units, 0:d_width],
                    preferred_element_type=jnp.float32,
                ).astype(jnp.bfloat16)
            for at in mine:
                later = at + t * per_target + slots

                @pl.when(later < d_tiles)
                def _():
                    down_copy(later).start()

            return carry

        lax.fori_loop(0, per_target // fours, down_step, 0)
        if t < ranks - 1:
            copy = to_peer(
                mlp_part.at[t], mlp_box.at[t], mlp_send.at[t], mlp_recv.at[t], peers[t]
            )
            copy.start()
            sends.append(copy)
    mlp_sum = mlp_part[ranks - 1].astype(jnp.float32)
    for t in range(ranks - 1):
        pltpu.make_async_copy(mlp_box.at[t], mlp_box.at[t], mlp_recv.at[t]).wait()
        mlp_sum = mlp_sum + mlp_box[t].astype(jnp.float32)
    layer_ref[...] = (tok_all[:, own_columns].astype(jnp.float32) + mlp_sum).astype(jnp.bfloat16)

    layer_copy = pltpu.make_async_copy(layer_ref, layer_out, out_sem.at[1])
    layer_copy.start()
    for copy in sends:
        copy.wait_send()

    def settle(key, carry):
        for piece in range(kv_heads):
            sent = q_all.at[0, pl.ds(piece * shared, shared)]
            pltpu.make_async_copy(sent, sent, q_send.at[piece, key]).wait()
            for source, out_sem in ((part, part_send), (stat, stat_send)):
                sent = source.at[0, piece]
                pltpu.make_async_copy(sent, sent, out_sem.at[piece, key]).wait()
        return carry

    lax.fori_loop(1, groups, settle, 0)
    context_copy.wait()
    layer_copy.wait()


def finish_kernel(context_ref, layer_ref, context_out, layer_out, buf_a, buf_b, sems):
    pairs = ((context_ref, buf_a, context_out), (layer_ref, buf_b, layer_out))
    for i, (source, buf, _) in enumerate(pairs):
        pltpu.make_async_copy(source, buf, sems.at[i]).start()
    for i, (source, buf, target) in enumerate(pairs):
        pltpu.make_async_copy(source, buf, sems.at[i]).wait()
        pltpu.make_async_copy(buf, target, sems.at[i]).start()
    for i, (_, buf, target) in enumerate(pairs):
        pltpu.make_async_copy(buf, target, sems.at[i]).wait()


def layer(groups, ranks, small, gains, tokens, weights, kv_pool):
    lengths, serving, owners, page_slots, inverse = small
    rows, share = tokens.shape
    model = share * ranks
    _, _, kv_heads, page, width = kv_pool.shape
    pages_max = owners.shape[1]
    per_owner = (pages_max + groups - 1) // groups
    span = (pages_max + 127) // 128 * 128
    heads = weights[0].shape[1] // width
    units = weights[4].shape[1]
    shared = heads // kv_heads
    bf16 = jnp.bfloat16
    f32 = jnp.float32
    i32 = jnp.int32
    dma = pltpu.SemaphoreType.DMA
    vmem = pl.BlockSpec(memory_space=VMEM)
    smem = pl.BlockSpec(memory_space=pltpu.SMEM)
    hbm = pl.BlockSpec(memory_space=pl.ANY)
    outs = (
        jax.ShapeDtypeStruct((rows, heads * width), bf16),
        jax.ShapeDtypeStruct((rows, share), bf16),
    )
    buffers = [
        (kv_pool.shape, bf16),
        ((rows, model), bf16),
        ((rows, model), bf16),
        ((groups, heads, rows, width), bf16),
        ((kv_heads, rows, width), bf16),
        ((kv_heads, rows, width), bf16),
        ((groups, kv_heads, shared, width, rows), bf16),
        ((groups, kv_heads, 2 * shared, rows), f32),
        ((kv_heads, groups, shared, width, rows), bf16),
        ((kv_heads, groups, 2 * shared, rows), f32),
        ((ranks, rows, model), bf16),
        ((rows, units), bf16),
        ((ranks, rows, share), bf16),
        ((ranks, rows, share), bf16),
        ((rows, heads * width), bf16),
        ((rows, share), bf16),
        ((rows, width), f32),
        ((rows, width), f32),
        ((1, width), f32),
        ((1, model), f32),
        ((1, model), f32),
        (owners.shape, i32),
        (owners.shape, i32),
        ((groups, span), i32),
        ((groups, span), i32),
        ((groups, span), i32),
        ((groups, span), i32),
    ]
    used = sum(math.prod(shape) * jnp.dtype(kind).itemsize for shape, kind in buffers)
    used += 64 * model + 2_500_000
    slots = (VMEM_BUDGET - used) // (2 * model * TILE) // 2 * 2
    found = pl.pallas_call(
        functools.partial(layer_kernel, (groups, ranks, kv_heads, per_owner)),
        out_shape=outs,
        in_specs=[smem, smem] + [hbm] * 14,
        out_specs=(hbm, hbm),
        scratch_shapes=[VMEM((slots, model, TILE), bf16)]
        + [VMEM(shape, kind) for shape, kind in buffers]
        + [
            pltpu.SMEM((groups, span), i32),
            dma((5,)),
            dma,
            dma((2,)),
            dma((slots,)),
            dma,
            dma,
            dma((ranks,)),
            dma((ranks,)),
            dma((kv_heads, groups)),
            dma((kv_heads, groups)),
            dma((kv_heads, groups)),
            dma((kv_heads, groups)),
            dma((kv_heads, groups)),
            dma((kv_heads, groups)),
            dma((ranks, 8)),
            dma((ranks, 8)),
            dma((ranks,)),
            dma((ranks,)),
        ],
        compiler_params=pltpu.CompilerParams(
            collective_id=0, has_side_effects=True, vmem_limit_bytes=67_000_000
        ),
        name="layer",
    )(lengths, serving, owners, page_slots, inverse, *gains, tokens, *weights, kv_pool)
    return pl.pallas_call(
        finish_kernel,
        out_shape=outs,
        in_specs=[hbm, hbm],
        out_specs=(hbm, hbm),
        scratch_shapes=[VMEM(out.shape, out.dtype) for out in outs] + [dma((2,))],
        name="finish",
    )(*found)


def shards(
    tokens,
    norm_gain,
    w_query,
    w_key,
    w_value,
    w_out,
    mlp_gain,
    w_gate,
    w_up,
    w_down,
    kv_pool,
    prefix_len,
    page_owner,
    page_slot,
    serving,
):
    width = kv_pool.shape[4]
    half = np.arange(width // 2)
    inverse = (THETA ** (-2.0 * half / width)).astype(np.float32)
    inverse = jnp.asarray(np.concatenate([inverse, inverse])[None, :])
    return layer(
        lax.axis_size("dp"),
        lax.axis_size("tp"),
        (prefix_len, serving, page_owner, page_slot, inverse),
        (norm_gain[None, :], mlp_gain[None, :]),
        tokens,
        (w_query, w_key, w_value, w_out, w_gate, w_up, w_down),
        kv_pool,
    )


def solution(mesh):
    in_specs = (
        P("dp", "tp"),
        P(),
        P(None, "tp"),
        P(None, "tp"),
        P(None, "tp"),
        P("tp", None),
        P(),
        P(None, "tp"),
        P(None, "tp"),
        P("tp", None),
        P("dp", None, "tp", None, None),
        P(),
        P(),
        P(),
        P(),
    )
    out_specs = (P("dp", "tp"), P("dp", "tp"))
    return jax.shard_map(shards, mesh=mesh, in_specs=in_specs, out_specs=out_specs, check_vma=False)
```

```python
import functools
import math

import jax
import jax.numpy as jnp
import numpy as np
from jax import lax
from jax.experimental import pallas as pl
from jax.experimental.pallas import tpu as pltpu
from jax.sharding import PartitionSpec as P

EPS = 1e-05
THETA = 500000.0
NEG = -1e30
LOG2E = 1.4426950408889634
MESH = pl.DeviceIdType.MESH
VMEM = pltpu.VMEM
VMEM_BUDGET = 66_800_000
TILE = 256


def xor(a, b, bits):
    out = 0
    for bit in range(bits):
        unit = 1 << bit
        out = out + lax.rem(lax.div(a, unit) + lax.div(b, unit), 2) * unit
    return out


TUNED = (
    "C0", "I0.2", "I0.1", "I2.12", "C1", "I1.2", "I3.4", "I1.1", "I0.12", "I1.4", "I2.1", "C2",
    "I3.2", "F0.1", "I3.1", "I3.12", "F3.4", "F2.12", "I0.4", "F1.1", "I2.2", "I1.12", "F1.4",
    "F0.12", "I2.4", "F0.4", "F3.12", "F3.1", "F1.12", "F3.6", "F2.1", "F2.4", "I0.8", "F0.13",
    "A12", "F1.5", "F2.5", "I1.8", "F3.5", "F0.6", "F2.6", "F3.14", "F1.13", "F0.5", "F0.15",
    "F1.14", "F0.14", "F2.14", "F1.6", "F3.13", "F2.13", "A6", "R2.6", "F0.8", "F3.7", "F1.7",
    "I2.8", "I3.8", "F2.7", "R0.6", "A14", "R1.6", "F1.15", "A0", "R2.14", "F0.7", "F1.8",
    "F1.2", "F2.15", "F3.15", "F0.2", "R1.14", "F2.9", "R3.14", "A15", "A13", "R1.15", "F2.2",
    "F3.2", "F2.8", "A4", "R2.15", "R0.15", "A2", "M2.12", "F1.9", "M1.12", "R3.15", "F0.9",
    "M3.12", "F0.3", "N2.12", "F3.8", "M2.13", "F3.9", "A8", "F2.3", "M1.13", "R3.2", "N2.13",
    "N3.12", "A7", "M0.13", "R0.14", "R3.6", "A5", "M3.13", "F0.11", "N3.13", "N1.12", "F2.11",
    "R3.7", "F3.11", "F1.3", "R2.7", "R0.7", "F0.10", "F1.10", "F3.10", "F2.10", "F1.11", "A11",
    "R3.11", "R0.11", "A10", "R2.11", "F3.3", "R1.10", "M0.12", "M2.5", "N0.12", "R3.10", "A9",
    "R1.11", "R2.10", "A3", "R1.7", "M3.5", "R0.2", "M0.9", "R0.10", "M1.4", "M2.4", "M0.4",
    "M3.8", "M2.9", "M0.5", "N2.4", "N2.9", "M3.4", "R0.3", "N2.5", "R2.3", "R3.3", "M3.9",
    "R1.3", "R1.2", "N3.8", "M1.8", "M2.8", "N3.5", "M1.9", "R2.2", "N2.8", "N3.4", "A1",
    "N3.9", "M0.8", "N0.8", "M0.0", "M3.0", "M0.1", "M1.5", "N0.4", "N3.0", "M3.1", "N1.8",
    "M2.1", "N3.1", "M1.1", "M2.0", "N1.4", "M1.0", "N2.0", "N2.1", "N0.0", "N1.0",
)


def schedule(planes):
    if planes == 4:
        return [(word[0], [int(part) for part in word[1:].split(".")]) for word in TUNED]
    routes = range(4)
    tasks = []
    for piece in range(2):
        tasks.append(("C", [piece]))
        keys = [1, 2] + [4 * j for j in range(1, planes)]
        tasks += [("I", [route, key]) for key in keys for route in (piece, piece + 2)]
    tasks.append(("C", [2]))
    for key in range(4 * planes):
        tasks += [("F", [route, key]) for route in routes if key]
        tasks.append(("A", [key]))
        tasks += [("R", [route, key]) for route in routes if key % 4 >= 2]
    for j in reversed(range(planes)):
        tasks += [("M", [route, 4 * j + turn]) for turn in (1, 0) for route in routes]
    for j in reversed(range(planes)):
        tasks += [("N", [route, 4 * j]) for route in routes]
        tasks += [("N", [route, 4 * j + 1]) for route in (2, 3)]
    return tasks


def flipped(me, mask):
    out = me
    bit = 1
    while bit <= mask:
        if mask & bit:
            out = out + (1 - 2 * lax.rem(lax.div(me, bit), 2)) * bit
        bit *= 2
    return out


def merge_stats(left, right):
    top = jnp.maximum(left[0:1], right[0:1])
    factor_left = jnp.exp2(left[0:1] - top)
    factor_right = jnp.exp2(right[0:1] - top)
    count = left[1:2] * factor_left + right[1:2] * factor_right
    return jnp.concatenate([top, count], axis=0), factor_left, factor_right


def layer_kernel(
    plan,
    length_ref,
    serving_ref,
    owner_ref,
    page_slot_ref,
    inverse_ref,
    norm_gain_ref,
    mlp_norm_gain_ref,
    tokens_ref,
    wq_ref,
    wk_ref,
    wv_ref,
    wo_ref,
    wg_ref,
    wu_ref,
    wd_ref,
    kv_ref,
    context_out,
    layer_out,
    ring,
    kv_buf,
    tok_all,
    normed,
    q_all,
    new_k,
    new_v,
    part,
    stat,
    box,
    stat_box,
    attn_all,
    hidden,
    mlp_part,
    mlp_box,
    context_ref,
    layer_ref,
    cos_ref,
    sin_ref,
    inverse_buf,
    gain_ref,
    mlp_gain_ref,
    owner_buf,
    page_slot_buf,
    owner_rows,
    slot_rows,
    length_rows,
    picks,
    picked,
    small_sem,
    picks_sem,
    out_sem,
    ring_sem,
    kv_sem,
    tok_sem,
    tok_send,
    tok_recv,
    q_send,
    q_recv,
    part_send,
    part_recv,
    stat_send,
    stat_recv,
    attn_send,
    attn_recv,
    mlp_send,
    mlp_recv,
):
    groups, ranks, kv_heads, per_owner = plan
    me = lax.axis_index("dp")
    rank = lax.axis_index("tp")
    bits = groups.bit_length() - 1
    planes = groups // 4
    rows, model = normed.shape
    share = tokens_ref.shape[1]
    width = q_all.shape[3]
    heads = q_all.shape[1]
    shared = heads // kv_heads
    page = kv_ref.shape[3]
    slots = ring.shape[0]
    units = wd_ref.shape[0]
    own_rows = wo_ref.shape[0]
    peers = [lax.rem(rank + 1 + t, ranks) for t in range(ranks - 1)]

    def slabs(total):
        step = math.gcd(total, TILE)
        return step, total // step

    q_width, q_tiles = slabs(wq_ref.shape[1])
    k_width, k_tiles = slabs(wk_ref.shape[1])
    g_width, g_tiles = slabs(units)
    d_width, d_tiles = slabs(share)
    d_tiles = d_tiles * ranks
    o_stack = model // own_rows
    o_cols = o_stack * TILE
    o_tiles = model // o_cols
    first_k = q_tiles
    first_v = first_k + k_tiles
    first_o = first_v + k_tiles
    first_g = first_o + o_tiles
    first_d = first_g + 2 * g_tiles
    last = first_d + d_tiles

    def slot_of(tile):
        return tile % slots if isinstance(tile, int) else lax.rem(tile, slots)

    def column_copy(source, start, step, tile):
        slot = slot_of(tile)
        count = source.shape[0]
        columns = pl.ds(pl.multiple_of(start, step), step)
        return pltpu.make_async_copy(
            source.at[:, columns],
            ring.at[slot, pl.ds(0, count), pl.ds(0, step)],
            ring_sem.at[slot],
        )

    def q_copy(i):
        return column_copy(wq_ref, i * q_width, q_width, i)

    def k_copy(i):
        return column_copy(wk_ref, i * k_width, k_width, first_k + i)

    def v_copy(i):
        return column_copy(wv_ref, i * k_width, k_width, first_v + i)

    def gate_copy(i, which):
        return column_copy((wg_ref, wu_ref)[which], i * g_width, g_width, first_g + 2 * i + which)

    def down_copy(i):
        per = d_tiles // ranks
        target = lax.rem(rank + 1 + i // per, ranks)
        return column_copy(wd_ref, target * share + (i % per) * d_width, d_width, first_d + i)

    def out_start(i):
        slot = slot_of(first_o + i)
        for s in range(o_stack):
            pltpu.make_async_copy(
                wo_ref.at[:, pl.ds(i * o_cols + s * TILE, TILE)],
                ring.at[slot, pl.ds(s * own_rows, own_rows), :],
                ring_sem.at[slot],
            ).start()

    def out_wait(i):
        slot = slot_of(first_o + i)
        pltpu.make_async_copy(ring.at[slot], ring.at[slot], ring_sem.at[slot]).wait()

    def start_tile(tile):
        if tile >= last:
            return
        if tile < first_k:
            q_copy(tile).start()
        elif tile < first_v:
            k_copy(tile - first_k).start()
        elif tile < first_o:
            v_copy(tile - first_v).start()
        elif tile < first_g:
            out_start(tile - first_o)
        elif tile < first_d:
            gate_copy((tile - first_g) // 2, (tile - first_g) % 2).start()
        else:
            down_copy(tile - first_d).start()

    own_columns = pl.ds(pl.multiple_of(rank * share, share), share)
    own_load = pltpu.make_async_copy(tokens_ref, tok_all.at[:, own_columns], tok_sem)
    own_load.start()
    small = [
        pltpu.make_async_copy(source, target, small_sem.at[i])
        for i, (source, target) in enumerate(
            (
                (norm_gain_ref, gain_ref),
                (inverse_ref, inverse_buf),
                (owner_ref, owner_buf),
                (page_slot_ref, page_slot_buf),
                (mlp_norm_gain_ref, mlp_gain_ref),
            )
        )
    ]
    for copy in small:
        copy.start()
    for tile in range(first_o):
        start_tile(tile)

    x_to = me + 1 - 2 * lax.rem(me, 2)
    y_to = me + 2 - 4 * lax.rem(lax.div(me, 2), 2)
    hops = ((x_to, y_to), (y_to, x_to))

    barrier = pltpu.get_barrier_semaphore()
    for peer in peers:
        pl.semaphore_signal(barrier, inc=1, device_id={"tp": peer}, device_id_type=MESH)
    near = [x_to, y_to] + [xor(me, 4 * j, bits) for j in range(1, planes)]
    for other in near:
        pl.semaphore_signal(barrier, inc=1, device_id={"dp": other}, device_id_type=MESH)
    own_load.wait()
    pl.semaphore_wait(barrier, len(near) + len(peers))

    def to_peer(source, target, send_sem, recv_sem, peer):
        return pltpu.make_async_remote_copy(
            src_ref=source,
            dst_ref=target,
            send_sem=send_sem,
            recv_sem=recv_sem,
            device_id={"tp": peer},
            device_id_type=MESH,
        )

    sends = []
    for t, peer in enumerate(peers):
        copy = to_peer(
            tokens_ref,
            tok_all.at[:, own_columns],
            tok_send.at[t],
            tok_recv.at[t],
            peer,
        )
        copy.start()
        sends.append(copy)
    kv_load = pltpu.make_async_copy(kv_ref, kv_buf, kv_sem)
    for copy in small:
        copy.wait()

    length = length_ref[serving_ref[me]]
    position = length + lax.broadcasted_iota(jnp.int32, (rows, width), 0)
    angles = position.astype(jnp.float32) * inverse_buf[...]
    lane = lax.broadcasted_iota(jnp.int32, (rows, width), 1)
    cos_ref[...] = jnp.cos(angles)
    sine = jnp.sin(angles)
    sin_ref[...] = jnp.where(lane < width // 2, -sine, sine)

    pages_max = owner_buf.shape[1]
    span = owner_rows.shape[1]

    def group_row(group, carry):
        request = serving_ref[group]
        here = pl.ds(group, 1)
        owner_rows[here, 0:pages_max] = owner_buf[pl.ds(request, 1), :]
        slot_rows[here, 0:pages_max] = page_slot_buf[pl.ds(request, 1), :]
        length_rows[here, :] = jnp.full((1, span), length_ref[request], jnp.int32)
        return carry

    lax.fori_loop(0, groups, group_row, 0)
    lane = lax.broadcasted_iota(jnp.int32, (groups, span), 1)
    owned = ((owner_rows[...] == me) & (lane < pages_max)).astype(jnp.int32)
    before = owned
    shift = 1
    while shift < span:
        before = before + jnp.where(lane >= shift, pltpu.roll(before, shift, 1), 0)
        shift *= 2
    before = before - owned
    left = jnp.clip(length_rows[...] - lane * page, 0, page)
    table = jnp.zeros((groups, span), jnp.int32)
    for k in range(per_owner):
        chosen = (owned > 0) & (before == k)
        for at, source in ((k, slot_rows[...]), (per_owner + k, left)):
            value = jnp.sum(jnp.where(chosen, source, 0), axis=1, keepdims=True)
            table = table + jnp.where(lane == at, value, 0)
    picks[...] = table
    picks_copy = pltpu.make_async_copy(picks, picked, picks_sem)
    picks_copy.start()

    for t in range(ranks - 1):
        came = lax.rem(rank + 2 * ranks - 1 - t, ranks)
        landed = tok_all.at[:, pl.ds(pl.multiple_of(came * share, share), share)]
        pltpu.make_async_copy(landed, landed, tok_recv.at[t]).wait()

    def normalize(gain):
        squares = jnp.zeros((rows, 1), jnp.float32)
        for start in range(0, model, share):
            piece = tok_all[:, start : start + share].astype(jnp.float32)
            squares = squares + jnp.sum(piece * piece, axis=-1, keepdims=True)
        factor = lax.rsqrt(squares / model + EPS)
        for start in range(0, model, share):
            piece = tok_all[:, start : start + share].astype(jnp.float32)
            normed[:, start : start + share] = (
                piece * factor * gain[:, start : start + share]
            ).astype(jnp.bfloat16)

    normalize(gain_ref)

    def rope(values):
        return values * cos_ref[...] + pltpu.roll(values, width // 2, 1) * sin_ref[...]

    minor = shared // 4
    parts_of = ((0, shared - minor), (shared - minor, minor))

    def send_query(route, block, target, key):
        start, size = parts_of[route // 2]
        cut = pl.ds((route % 2) * shared + start, size)
        pltpu.make_async_remote_copy(
            src_ref=q_all.at[block, cut],
            dst_ref=q_all.at[block, cut],
            send_sem=q_send.at[route, key],
            recv_sem=q_recv.at[route, key],
            device_id={"dp": target},
            device_id_type=MESH,
        ).start()

    def block_of(piece, key):
        if piece % 2:
            low = lax.rem(key, 4)
            key = key - low + lax.div(low, 2) + 2 * lax.rem(low, 2)
        return xor(me, key, bits)

    def block_at(piece, key):
        low = key % 4
        if piece % 2:
            low = low // 2 + 2 * (low % 2)
        return flipped(me, key - key % 4 + low)

    tiles_each = q_tiles // kv_heads
    per_tile = q_width // width

    def project(piece):
        tiles = [piece * tiles_each + t for t in range(tiles_each)]
        for tile in tiles:
            q_copy(tile).wait()
        for tile in tiles:
            values = jnp.dot(
                normed[...], ring[tile, :, 0:q_width], preferred_element_type=jnp.float32
            )
            for h in range(per_tile):
                q_all[me, tile * per_tile + h] = rope(
                    values[:, h * width : (h + 1) * width]
                ).astype(jnp.bfloat16)

    def send_own(route, key):
        target = hops[route % 2][key - 1] if key < 4 else flipped(me, key)
        send_query(route, me, target, key)

    def forward(route, key):
        block = block_at(route % 2, key)
        near_to, far_to = hops[route % 2]
        start, size = parts_of[route // 2]
        landed = q_all.at[block, pl.ds((route % 2) * shared + start, size)]
        pltpu.make_async_copy(landed, landed, q_recv.at[route, key]).wait()
        if route >= 2 and key == 1:
            for j in sorted(range(1, planes), key=lambda j: abs(j - 2) * 2 + j // 3):
                send_query(route, block, flipped(me, 4 * j), 4 * j + 1)
        if route < 2 and key % 4 == 0:
            send_query(route, block, near_to, key + 1)
        if key % 4 < 2:
            send_query(route, block, far_to, key + 2)

    tasks = [
        (kind, spec)
        for kind, spec in schedule(planes)
        if kind in "CA" or spec[0] % 2 < kv_heads
    ]
    marks = [tasks.index(("C", [at])) for at in range(3)]
    for at in range(2):
        if at < kv_heads:
            project(at)
        if at == 0:
            kv_load.start()
        for kind, spec in tasks[marks[at] + 1 : marks[at + 1]]:
            (send_own if kind == "I" else forward)(*spec)
    tasks = tasks[marks[2] + 1 :]

    for i in range(k_tiles):
        k_copy(i).wait()
        v_copy(i).wait()
    per_tile = k_width // width
    for i in range(k_tiles):
        for first, store, turn in ((first_k, new_k, rope), (first_v, new_v, lambda v: v)):
            values = jnp.dot(
                normed[...], ring[first + i, :, 0:k_width], preferred_element_type=jnp.float32
            )
            for h in range(per_tile):
                store[i * per_tile + h] = turn(values[:, h * width : (h + 1) * width]).astype(
                    jnp.bfloat16
                )
    for tile in range(first_o, slots + first_o):
        start_tile(tile)
    kv_load.wait()
    picks_copy.wait()

    scale = LOG2E / math.sqrt(width)

    def attend(keys, values, ok, block, piece):
        queries = q_all[block, piece * shared : (piece + 1) * shared]
        queries = queries.reshape(shared * rows, width)
        scores = lax.dot_general(
            keys, queries, (((1,), (1,)), ((), ())), preferred_element_type=jnp.float32
        )
        scores = jnp.where(ok, scores * scale, NEG)
        highest = jnp.max(scores, axis=0, keepdims=True)
        expo = jnp.exp2(scores - highest)
        count = jnp.sum(expo, axis=0, keepdims=True)
        summed = lax.dot_general(
            values,
            expo.astype(jnp.bfloat16),
            (((0,), (0,)), ((), ())),
            preferred_element_type=jnp.float32,
        )
        return highest, count, summed

    def keep(found, part_to, stat_to):
        highest, count, summed = found
        for j in range(shared):
            lanes = slice(j * rows, (j + 1) * rows)
            part_to[j] = summed[:, lanes].astype(jnp.bfloat16)
            stat_to[j, 0:1] = highest[:, lanes]
            stat_to[j, 1:2] = count[:, lanes]

    key_row = lax.broadcasted_iota(jnp.int32, (rows, shared * rows), 0)
    token = lax.rem(lax.broadcasted_iota(jnp.int32, (rows, shared * rows), 1), rows)
    for piece in range(kv_heads):
        keep(
            attend(new_k[piece], new_v[piece], key_row <= token, me, piece),
            box.at[piece, 0],
            stat_box.at[piece, 0],
        )

    def send_part(route, block, target, key):
        piece = route % 2
        cut = pl.ds(*parts_of[route // 2])
        for source, target_box, out_sem, in_sem in (
            (part, box, part_send, part_recv),
            (stat, stat_box, stat_send, stat_recv),
        ):
            pltpu.make_async_remote_copy(
                src_ref=source.at[block, piece, cut],
                dst_ref=target_box.at[piece, key, cut],
                send_sem=out_sem.at[route, key],
                recv_sem=in_sem.at[route, key],
                device_id={"dp": target},
                device_id_type=MESH,
            ).start()

    def landed_part(route, key):
        cut = pl.ds(*parts_of[route // 2])
        for target_box, in_sem in ((box, part_recv), (stat_box, stat_recv)):
            landed = target_box.at[route % 2, key, cut]
            pltpu.make_async_copy(landed, landed, in_sem.at[route, key]).wait()

    row = lax.broadcasted_iota(jnp.int32, (page, 1), 0)

    def merge_into(route, block, key):
        landed_part(route, key)
        piece = route % 2
        start, size = parts_of[route // 2]
        for j in range(start, start + size):
            merged, mine, other = merge_stats(stat[block, piece, j], stat_box[piece, key, j])
            part[block, piece, j] = (
                part[block, piece, j].astype(jnp.float32) * mine
                + box[piece, key, j].astype(jnp.float32) * other
            ).astype(jnp.bfloat16)
            stat[block, piece, j] = merged

    def run_task(kind, route, key):
        near_to, far_to = hops[route % 2]
        block = block_at(route % 2, key)
        if kind == "I":
            send_own(route, key)
        elif kind == "F":
            forward(route, key)
        elif kind == "R":
            send_part(route, block, far_to, key)
        elif kind == "M":
            merge_into(route, block, key + 2)
            if route < 2 and key % 4 == 1:
                send_part(route, block, near_to, key)
        elif kind == "N":
            if route < 2:
                merge_into(route, block, key + 1)
            if key >= 4:
                send_part(route, block, flipped(me, key - key % 4), key)
            elif key == 1:
                for j in range(1, planes):
                    merge_into(route, block, 4 * j + 1)
                send_part(route, block, near_to, 1)

    before_turn = [[]]
    order = []
    for kind, spec in tasks:
        if kind == "A":
            order.append(spec[0])
            before_turn.append([])
        else:
            before_turn[-1].append((kind, *spec))

    def one_turn(turn, carry):
        for at, todo in enumerate(before_turn[:-1]):
            if todo:

                @pl.when(turn == at)
                def _():
                    for task in todo:
                        run_task(*task)

        key = 0
        for at, value in enumerate(order):
            key = jnp.where(turn == at, value, key)
        for piece in range(kv_heads):
            block = block_of(piece, key)
            pages = [picked[block, k] for k in range(per_owner)]
            ok = jnp.concatenate(
                [row < picked[block, per_owner + k] for k in range(per_owner)], axis=0
            )
            keys = jnp.concatenate([kv_buf[p, 0, piece] for p in pages], axis=0)
            values = jnp.concatenate([kv_buf[p, 1, piece] for p in pages], axis=0)
            keep(
                attend(keys, values, ok, block, piece),
                part.at[block, piece],
                stat.at[block, piece],
            )
        return carry

    lax.fori_loop(0, groups, one_turn, 0)
    for task in before_turn[-1]:
        run_task(*task)

    for piece in range(kv_heads):

        def fold(held, total, key, h):
            merged, mine, other = merge_stats(held, stat_box[piece, key, h])
            return merged, total * mine + box[piece, key, h].astype(jnp.float32) * other

        def home_merge(j, carry, piece=piece, fold=fold):
            @pl.when(j > 0)
            def _():
                landed_part(piece, 4 * j)
                landed_part(piece + 2, 4 * j)

            folded = [fold(carry[2 * h], carry[2 * h + 1], 4 * j, h) for h in range(shared)]
            return tuple(item for pair in folded for item in pair)

        start = []
        for h in range(shared):
            start += [stat[me, piece, h], part[me, piece, h].astype(jnp.float32)]
        done = list(lax.fori_loop(0, planes, home_merge, tuple(start)))
        landed_part(piece + 2, 1)
        for h in range(shared - minor, shared):
            done[2 * h : 2 * h + 2] = fold(done[2 * h], done[2 * h + 1], 1, h)
        for h in range(shared):
            lanes = slice((piece * shared + h) * width, (piece * shared + h + 1) * width)
            context_ref[:, lanes] = (done[2 * h + 1] / done[2 * h][1:2]).T.astype(jnp.bfloat16)

    context_copy = pltpu.make_async_copy(context_ref, context_out, out_sem.at[0])
    context_copy.start()
    for i in range(o_tiles):
        out_wait(i)
        for s in range(o_stack):
            start = i * o_cols + s * TILE
            attn_all[rank, :, start : start + TILE] = jnp.dot(
                context_ref[...],
                ring[slot_of(first_o + i), s * own_rows : (s + 1) * own_rows, :],
                preferred_element_type=jnp.float32,
            ).astype(jnp.bfloat16)
        start_tile(first_o + i + slots)
        for t, peer in enumerate(peers):
            ready = attn_all.at[rank, :, pl.ds(i * o_cols, o_cols)]
            copy = to_peer(ready, ready, attn_send.at[t, i], attn_recv.at[t, i], peer)
            copy.start()
            sends.append(copy)
    for i in range(o_tiles):
        columns = pl.ds(i * o_cols, o_cols)
        for t in range(ranks - 1):
            landed = attn_all.at[lax.rem(rank + 2 * ranks - 1 - t, ranks), :, columns]
            pltpu.make_async_copy(landed, landed, attn_recv.at[t, i]).wait()
        attn_sum = attn_all[0, :, columns].astype(jnp.float32)
        for r in range(1, ranks):
            attn_sum = attn_sum + attn_all[r, :, columns].astype(jnp.float32)
        tok_all[:, columns] = (tok_all[:, columns].astype(jnp.float32) + attn_sum).astype(
            jnp.bfloat16
        )

    normalize(mlp_gain_ref)

    pairs = math.gcd(g_tiles, 2)

    def gate_step(index, carry):
        mine = [index * pairs + u for u in range(pairs)]
        for i in mine:
            gate_copy(i, 0).wait()
            gate_copy(i, 1).wait()
        for i in mine:
            gate, up = [
                jnp.dot(
                    normed[...],
                    ring[slot_of(first_g + 2 * i + which), :, 0:g_width],
                    preferred_element_type=jnp.float32,
                )
                for which in range(2)
            ]
            columns = pl.ds(pl.multiple_of(i * g_width, g_width), g_width)
            hidden[:, columns] = (gate / (1.0 + jnp.exp(-gate)) * up).astype(jnp.bfloat16)
        for i in mine:
            later = i + slots // 2

            @pl.when(later < g_tiles)
            def _():
                gate_copy(later, 0).start()
                gate_copy(later, 1).start()

            for which in range(2):
                down = 2 * (later - g_tiles) + which

                @pl.when((later >= g_tiles) & (down < d_tiles))
                def _():
                    down_copy(down).start()

        return carry

    lax.fori_loop(0, g_tiles // pairs, gate_step, 0)

    per_target = d_tiles // ranks
    fours = math.gcd(per_target, 4)
    for t in range(ranks):

        def down_step(index, carry, t=t):
            mine = [index * fours + u for u in range(fours)]
            for at in mine:
                down_copy(at + t * per_target).wait()
            for at in mine:
                columns = pl.ds(pl.multiple_of(at * d_width, d_width), d_width)
                mlp_part[t, :, columns] = jnp.dot(
                    hidden[...],
                    ring[slot_of(first_d + at + t * per_target), 0:units, 0:d_width],
                    preferred_element_type=jnp.float32,
                ).astype(jnp.bfloat16)
            for at in mine:
                later = at + t * per_target + slots

                @pl.when(later < d_tiles)
                def _():
                    down_copy(later).start()

            return carry

        lax.fori_loop(0, per_target // fours, down_step, 0)
        if t < ranks - 1:
            copy = to_peer(
                mlp_part.at[t], mlp_box.at[t], mlp_send.at[t], mlp_recv.at[t], peers[t]
            )
            copy.start()
            sends.append(copy)
    mlp_sum = mlp_part[ranks - 1].astype(jnp.float32)
    for t in range(ranks - 1):
        pltpu.make_async_copy(mlp_box.at[t], mlp_box.at[t], mlp_recv.at[t]).wait()
        mlp_sum = mlp_sum + mlp_box[t].astype(jnp.float32)
    layer_ref[...] = (tok_all[:, own_columns].astype(jnp.float32) + mlp_sum).astype(jnp.bfloat16)

    layer_copy = pltpu.make_async_copy(layer_ref, layer_out, out_sem.at[1])
    layer_copy.start()
    for copy in sends:
        copy.wait_send()

    def settle(key, carry):
        for route in range(4):
            piece = route % 2
            if piece >= kv_heads:
                continue
            start, size = parts_of[route // 2]
            sent = q_all.at[0, pl.ds(piece * shared + start, size)]
            pltpu.make_async_copy(sent, sent, q_send.at[route, key]).wait()
            for source, out_sem in ((part, part_send), (stat, stat_send)):
                sent = source.at[0, piece, pl.ds(start, size)]
                pltpu.make_async_copy(sent, sent, out_sem.at[route, key]).wait()
        return carry

    lax.fori_loop(1, groups, settle, 0)
    context_copy.wait()
    layer_copy.wait()


def finish_kernel(context_ref, layer_ref, context_out, layer_out, buf_a, buf_b, sems):
    pairs = ((context_ref, buf_a, context_out), (layer_ref, buf_b, layer_out))
    for i, (source, buf, _) in enumerate(pairs):
        pltpu.make_async_copy(source, buf, sems.at[i]).start()
    for i, (source, buf, target) in enumerate(pairs):
        pltpu.make_async_copy(source, buf, sems.at[i]).wait()
        pltpu.make_async_copy(buf, target, sems.at[i]).start()
    for i, (_, buf, target) in enumerate(pairs):
        pltpu.make_async_copy(buf, target, sems.at[i]).wait()


def layer(groups, ranks, small, gains, tokens, weights, kv_pool):
    lengths, serving, owners, page_slots, inverse = small
    rows, share = tokens.shape
    model = share * ranks
    _, _, kv_heads, page, width = kv_pool.shape
    pages_max = owners.shape[1]
    per_owner = (pages_max + groups - 1) // groups
    span = (pages_max + 127) // 128 * 128
    heads = weights[0].shape[1] // width
    units = weights[4].shape[1]
    shared = heads // kv_heads
    bf16 = jnp.bfloat16
    f32 = jnp.float32
    i32 = jnp.int32
    dma = pltpu.SemaphoreType.DMA
    vmem = pl.BlockSpec(memory_space=VMEM)
    smem = pl.BlockSpec(memory_space=pltpu.SMEM)
    hbm = pl.BlockSpec(memory_space=pl.ANY)
    outs = (
        jax.ShapeDtypeStruct((rows, heads * width), bf16),
        jax.ShapeDtypeStruct((rows, share), bf16),
    )
    buffers = [
        (kv_pool.shape, bf16),
        ((rows, model), bf16),
        ((rows, model), bf16),
        ((groups, heads, rows, width), bf16),
        ((kv_heads, rows, width), bf16),
        ((kv_heads, rows, width), bf16),
        ((groups, kv_heads, shared, width, rows), bf16),
        ((groups, kv_heads, shared, 2, rows), f32),
        ((kv_heads, groups, shared, width, rows), bf16),
        ((kv_heads, groups, shared, 2, rows), f32),
        ((ranks, rows, model), bf16),
        ((rows, units), bf16),
        ((ranks, rows, share), bf16),
        ((ranks, rows, share), bf16),
        ((rows, heads * width), bf16),
        ((rows, share), bf16),
        ((rows, width), f32),
        ((rows, width), f32),
        ((1, width), f32),
        ((1, model), f32),
        ((1, model), f32),
        (owners.shape, i32),
        (owners.shape, i32),
        ((groups, span), i32),
        ((groups, span), i32),
        ((groups, span), i32),
        ((groups, span), i32),
    ]
    used = sum(math.prod(shape) * jnp.dtype(kind).itemsize for shape, kind in buffers)
    used += 64 * model + 2_500_000
    slots = (VMEM_BUDGET - used) // (2 * model * TILE) // 2 * 2
    found = pl.pallas_call(
        functools.partial(layer_kernel, (groups, ranks, kv_heads, per_owner)),
        out_shape=outs,
        in_specs=[smem, smem] + [hbm] * 14,
        out_specs=(hbm, hbm),
        scratch_shapes=[VMEM((slots, model, TILE), bf16)]
        + [VMEM(shape, kind) for shape, kind in buffers]
        + [
            pltpu.SMEM((groups, span), i32),
            dma((5,)),
            dma,
            dma((2,)),
            dma((slots,)),
            dma,
            dma,
            dma((ranks,)),
            dma((ranks,)),
            dma((4, groups)),
            dma((4, groups)),
            dma((4, groups)),
            dma((4, groups)),
            dma((4, groups)),
            dma((4, groups)),
            dma((ranks, 8)),
            dma((ranks, 8)),
            dma((ranks,)),
            dma((ranks,)),
        ],
        compiler_params=pltpu.CompilerParams(
            collective_id=0, has_side_effects=True, vmem_limit_bytes=67_000_000
        ),
        name="layer",
    )(lengths, serving, owners, page_slots, inverse, *gains, tokens, *weights, kv_pool)
    return pl.pallas_call(
        finish_kernel,
        out_shape=outs,
        in_specs=[hbm, hbm],
        out_specs=(hbm, hbm),
        scratch_shapes=[VMEM(out.shape, out.dtype) for out in outs] + [dma((2,))],
        name="finish",
    )(*found)


def shards(
    tokens,
    norm_gain,
    w_query,
    w_key,
    w_value,
    w_out,
    mlp_gain,
    w_gate,
    w_up,
    w_down,
    kv_pool,
    prefix_len,
    page_owner,
    page_slot,
    serving,
):
    width = kv_pool.shape[4]
    half = np.arange(width // 2)
    inverse = (THETA ** (-2.0 * half / width)).astype(np.float32)
    inverse = jnp.asarray(np.concatenate([inverse, inverse])[None, :])
    return layer(
        lax.axis_size("dp"),
        lax.axis_size("tp"),
        (prefix_len, serving, page_owner, page_slot, inverse),
        (norm_gain[None, :], mlp_gain[None, :]),
        tokens,
        (w_query, w_key, w_value, w_out, w_gate, w_up, w_down),
        kv_pool,
    )


def solution(mesh):
    in_specs = (
        P("dp", "tp"),
        P(),
        P(None, "tp"),
        P(None, "tp"),
        P(None, "tp"),
        P("tp", None),
        P(),
        P(None, "tp"),
        P(None, "tp"),
        P("tp", None),
        P("dp", None, "tp", None, None),
        P(),
        P(),
        P(),
        P(),
    )
    out_specs = (P("dp", "tp"), P("dp", "tp"))
    return jax.shard_map(shards, mesh=mesh, in_specs=in_specs, out_specs=out_specs, check_vma=False)
```
